32 devices in a mesh: groups: 2 (over y), expert: 16 (over z, x, core), tensor: 1.
Axes of the slice: x: 2, y: 2, z: 4, core: 2. Of those that a mesh axis runs over, the one named last changes fastest.
Arguments:
- tokens: bfloat16 [64, 4096], P(('groups', 'expert')), parts along dimension 0, may hold values from -6 to 6
- expert_ids: int32 [64, 2], P(('groups', 'expert')), parts along dimension 0, may hold values from 0 to 3, all different within a row; in each aligned block of 2 rows (0 to 1, 2 to 3, ...) at most 2 rows name the same one
- gate_weights: float32 [64, 2], P(('groups', 'expert')), parts along dimension 0, may hold values from 0.2 to 1
- doc_ids: int32 [64], P(('groups', 'expert')), parts along dimension 0, may hold values from 0 to 3, never falling along the last dimension, each value on 1 to 16 neighbouring positions
- w_gate: bfloat16 [4096, 2048], P(None, ('expert', 'tensor')), may hold values from -0.09375 to 0.09375
- w_up: bfloat16 [4096, 2048], P(None, ('expert', 'tensor')), may hold values from -0.09375 to 0.09375
- w_down: bfloat16 [2048, 4096], P(('expert', 'tensor')), may hold values from -0.25 to 0.25
- w_score: float32 [4096], P('tensor'), may hold values from -0.375 to 0.375
Outputs:
- mixed: bfloat16 [64, 4096], P(('groups', 'expert'), 'tensor'), parts along dimension 0
- scores: float32 [8], P('groups'), parts along dimension 0
The draws below stay inside these ranges and needn't reach their ends.
There are 2 independent parts, one for each index of `groups`. The reference program is written for one: setup_inputs(seed, part) draws one part's arguments, and reference() takes and returns one part's arrays. A program takes and returns all parts, laid end to end along the dimension named above; an argument that names none is the same for every part. Nothing has to cross between parts.
Inputs may be any that keep to these rules, and one draw needn't show every extreme that they name: `expert_ids`: each row names two different experts. Among the rows of one device no expert is named more than 2 times, and in some devices' rows some expert exactly 2 times. `doc_ids`: document ids never fall along the tokens; every document holds 1 to 16 tokens, one exactly 16.
All inputs are finite; a program needn't handle non-finite values.
Results may differ from the reference program's by a relative error of at most 0.0057.
Values may be sent and summed in bfloat16 or wider, within the bound.
No kernel may reach another device: no remote copies, remote signals or barrier semaphores. Data moves between devices by JAX's collectives and lax.ppermute only.
A program may use at most 64 MiB of HBM per device.

```python
import math
import jax
import jax.numpy as jnp
import numpy as np
from jax import lax

D = 4096
H_DEV = 128
EXP_FLIGHT = 4
TOK_DEV = 2
CAP = 2
TOKENS = 32
DOCS = 4
DOC_MOST = 16
FF_WIN = 512


def shard_levels(rng, shape, cuts, low, high):
    factor_of = 1.0
    for axis_at, shards_of in cuts:
        draws = jax.random.uniform(jax.random.fold_in(jax.random.fold_in(rng, 6), axis_at), (shards_of,), jnp.float32, low / len(cuts), high / len(cuts))
        factor_of = factor_of * jnp.repeat(jnp.exp(draws), shape[axis_at] // shards_of).reshape((-1,) + (1,) * (len(shape) - 1 - axis_at))
    return factor_of


def length_profile(number_of, total, limit, skew):
    loads = [(1 << 20) // math.isqrt(grade ** skew) + 1 for grade in range(2, number_of + 1)]
    rest, given = total - limit - (number_of - 1), [1] * (number_of - 1)
    while rest > 0:
        candidates = [i for i in range(number_of - 1) if given[i] < limit]
        mass, budget = sum([loads[i] for i in candidates]), rest
        for i in candidates:
            extra = min(limit - given[i], max(1, budget * loads[i] // mass), rest)
            given[i] = given[i] + extra
            rest = rest - extra
    return np.array([limit] + given)


def ragged_sizes(stream_key, number_of, total, limit, skew):
    if number_of == 2:
        one = jax.random.randint(stream_key, (), max(1, total - limit), min(limit, total - 1) + 1)
        return jnp.stack([one, total - one])
    tallies = jnp.asarray(length_profile(number_of, total, limit, skew), jnp.int32)
    twos = (number_of - 1) // 2
    giver, sink = tallies[1:1 + 2 * twos:2], tallies[2:2 + 2 * twos:2]
    room = jnp.minimum(giver - 1, limit - sink)
    moved = jax.random.randint(jax.random.fold_in(stream_key, 1), (twos,), 0, 1 << 20) % (room + 1)
    tallies = tallies.at[1:1 + 2 * twos:2].set(giver - moved).at[2:2 + 2 * twos:2].set(sink + moved)
    return tallies[jax.random.permutation(jax.random.fold_in(stream_key, 2), number_of)]


def routed_block(key, own, number, rows, amount, top, limit, lean):
    sequence = jax.random.permutation(key, amount)
    packed, ordinary = shares(amount, rows * top, limit, lean, True), shares(amount, rows * top, limit, lean, False)
    places = jnp.arange(amount)

    def named(sizes, rotation):
        used = int((sizes > 0).sum())
        fixed = max(1, used // 4)
        moved = fixed + (places - fixed + rotation * (used - fixed)) % max(1, amount - fixed)
        return jnp.zeros((amount,), jnp.int32).at[sequence[jnp.where(places < fixed, places, moved)]].set(jnp.asarray(sizes, jnp.int32))

    sizes = jnp.where(number % 4 == 0, named(packed, number // 4), named(ordinary, number - number // 4 - 1))
    mixed = jax.random.permutation(jax.random.fold_in(own, 3), amount)
    source_of, taker = mixed[0:amount // 2 * 2:2], mixed[1:amount // 2 * 2:2]
    room = jnp.minimum(sizes[source_of] - 1, limit - sizes[taker]) // 2
    room = jnp.where((source_of == sequence[0]) | (taker == sequence[0]) | (sizes[taker] == 0), 0, jnp.maximum(room, 0))
    moved = jax.random.randint(jax.random.fold_in(own, 4), (amount // 2,), 0, 1 << 20) % (room + 1)
    sizes = sizes.at[source_of].add(-moved).at[taker].add(moved)
    labels = jnp.searchsorted(jnp.cumsum(sizes), jnp.arange(rows * top), side="right").astype(jnp.int32)
    table = labels.reshape(top, rows).T
    table = table[jax.random.permutation(jax.random.fold_in(own, 1), rows)]
    rotation = jax.random.randint(jax.random.fold_in(own, 2), (rows, 1), 0, top)
    return jnp.take_along_axis(table, (jnp.arange(top)[None, :] + rotation) % top, axis=1)


def shares(amount, total, most, skew, full):
    weights = [(1 << 20) // math.isqrt(grade ** skew) + 1 for grade in range(1, amount + 1)]
    largest = most if full else min(most, max(-(-total // amount), total * weights[0] // sum(weights)))
    least = 1 if total - largest >= amount - 1 else 0
    given, spare = [largest] + [least] * (amount - 1), total - largest - least * (amount - 1)
    while spare > 0:
        candidates = [i for i in range(1, amount) if given[i] < largest] or [i for i in range(1, amount) if given[i] < most]
        pool, budget = sum([weights[i] for i in candidates]), spare
        for i in candidates:
            extra = min(most - given[i], max(1, budget * weights[i] // pool), spare)
            given[i] = given[i] + extra
            spare = spare - extra
    return np.array(given)


def scatter_about(own_key, dims, scale, bound, pieces=(), held_as=jnp.bfloat16):
    result = jax.random.normal(own_key, dims, jnp.float32) * scale
    if len(pieces) > 0:
        result = shard_levels(own_key, dims, pieces, -0.22, 0.18) * result
    return jnp.clip(result, min=-bound, max=bound).astype(held_as)


def setup_inputs(seed: int = 0, part: int = 0) -> dict:
    arg_keys = jax.random.split(jax.random.key(seed), 9)
    part_keys = jax.random.split(jax.random.fold_in(arg_keys[8], part), 9)
    tokens = scatter_about(part_keys[0], (TOKENS, D), 1.0, 6.0, ((0, 16),))
    expert_ids_keys = jax.random.split(jax.random.fold_in(part_keys[1], 1), TOKENS // TOK_DEV)
    expert_ids_turns = jax.random.permutation(jax.random.fold_in(part_keys[1], 3), TOKENS // TOK_DEV)
    expert_ids = jax.vmap(lambda own, number: routed_block(jax.random.fold_in(part_keys[1], 2), own, number, TOK_DEV, EXP_FLIGHT, 2, CAP, 1))(expert_ids_keys, expert_ids_turns).reshape((TOKENS, 2))
    gate_weights = jnp.clip(jnp.exp(math.log(1.0) - 1.609438 * jax.random.uniform(part_keys[2], (TOKENS, 2), jnp.float32) ** shard_levels(part_keys[2], (TOKENS, 2), ((0, 16),), -0.2, 0.2)), 0.2, 1.0)
    doc_ids = jnp.searchsorted(jnp.cumsum(ragged_sizes(part_keys[3], DOCS, TOKENS, DOC_MOST, 1)), jnp.arange(TOKENS), side="right").astype(jnp.int32)
    w_gate = scatter_about(arg_keys[4], (D, EXP_FLIGHT * FF_WIN), D ** -0.5, 0.09375, ((1, 16),))
    w_up = scatter_about(arg_keys[5], (D, EXP_FLIGHT * FF_WIN), D ** -0.5, 0.09375, ((1, 16),))
    w_down = scatter_about(arg_keys[6], (EXP_FLIGHT * FF_WIN, D), FF_WIN ** -0.5, 0.25, ((0, 16),))
    w_score = scatter_about(arg_keys[7], (D,), (4.0 / D ** 0.5), 0.375, (), jnp.float32)
    return dict(tokens=tokens, expert_ids=expert_ids, gate_weights=gate_weights, doc_ids=doc_ids, w_gate=w_gate, w_up=w_up, w_down=w_down, w_score=w_score)


def reference(tokens, expert_ids, gate_weights, doc_ids, w_gate, w_up, w_down, w_score):
    width = tokens.shape[1]
    nblocks = FF_WIN // H_DEV
    mixed_acc = jnp.zeros((TOKENS, width), jnp.float32)
    for expert in range(EXP_FLIGHT):
        first = expert * FF_WIN
        gate_part = jnp.dot(tokens, w_gate[:, first:first + FF_WIN], preferred_element_type=jnp.float32)
        up_part = jnp.dot(tokens, w_up[:, first:first + FF_WIN], preferred_element_type=jnp.float32)
        hidden = (jax.nn.silu(gate_part) * up_part).astype(jnp.bfloat16)
        hidden_blocks = hidden.reshape(TOKENS, nblocks, H_DEV).transpose(1, 0, 2)
        down_blocks = w_down[first:first + FF_WIN].reshape(nblocks, H_DEV, width)

        def add_block(total, pair):
            piece = jnp.dot(pair[0], pair[1], preferred_element_type=jnp.float32).astype(jnp.bfloat16)
            piece = lax.optimization_barrier(piece)
            return total + piece.astype(jnp.float32), None

        expert_out, _ = lax.scan(add_block, jnp.zeros((TOKENS, width), jnp.float32), (hidden_blocks, down_blocks))
        weight = jnp.sum(jnp.where(expert_ids == expert, gate_weights, jnp.float32(0.0)), axis=1)
        mixed_acc = mixed_acc + weight[:, None] * expert_out
    mixed = mixed_acc.astype(jnp.bfloat16)
    projected = jnp.dot(mixed.astype(jnp.float32), w_score, precision=lax.Precision.HIGHEST)
    docs_hit = (doc_ids[:, None] == jnp.arange(DOCS, dtype=jnp.int32)[None, :]).astype(jnp.float32)
    totals = jnp.dot(projected, docs_hit, precision=lax.Precision.HIGHEST)
    counts = jnp.sum(docs_hit, axis=0)
    scores = jax.nn.sigmoid(totals / counts)
    return mixed, scores
```

```python
import jax
import jax.numpy as jnp
from jax import lax
from jax.sharding import PartitionSpec as P

EXP_FLIGHT = 4
LANES = 128
PIECES = 3


def split_wide(value):
    pieces = []
    rest = value
    for _ in range(PIECES):
        piece = lax.reduce_precision(rest, 8, 7)
        pieces.append(piece)
        rest = rest - piece
    return pieces


def side_lanes(columns, rows):
    lane = lax.broadcasted_iota(jnp.int32, (rows, LANES), 1)
    out = jnp.zeros((rows, LANES), jnp.float32)
    for at, column in enumerate(columns):
        out = jnp.where(lane == at, column, out)
    return out.astype(jnp.bfloat16)


def local(tokens, expert_ids, gate_weights, doc_ids, w_gate, w_up, w_down, w_score):
    members = lax.axis_size("expert")
    parts = lax.axis_size("tensor")
    tok_rows, width = tokens.shape
    rows = members * tok_rows
    spread = members // EXP_FLIGHT
    doc_total = rows // 8
    own_expert = lax.axis_index("expert") // spread

    columns = []
    for expert in range(EXP_FLIGHT):
        weight = jnp.sum(
            jnp.where(expert_ids == expert, gate_weights, jnp.float32(0.0)), axis=1, keepdims=True
        )
        columns += split_wide(weight)
    columns.append(doc_ids[:, None].astype(jnp.float32))
    outgoing = jnp.concatenate([tokens, side_lanes(columns, tok_rows)], axis=1)
    outgoing = jnp.broadcast_to(outgoing[None], (members, tok_rows, width + LANES))
    gathered = lax.all_to_all(outgoing, "expert", split_axis=0, concat_axis=0, tiled=True)
    gathered = gathered.reshape(rows, width + LANES)
    flat = gathered[:, :width]
    side = gathered[:, width:].astype(jnp.float32)

    gate_part = jnp.dot(flat, w_gate, preferred_element_type=jnp.float32)
    up_part = jnp.dot(flat, w_up, preferred_element_type=jnp.float32)
    hidden = (jax.nn.silu(gate_part) * up_part).astype(jnp.bfloat16)
    partial_value = jnp.dot(hidden, w_down, preferred_element_type=jnp.float32)

    lane = lax.broadcasted_iota(jnp.int32, (rows, LANES), 1)
    mine = (lane >= own_expert * PIECES) & (lane < (own_expert + 1) * PIECES)
    weight = jnp.sum(jnp.where(mine, side, jnp.float32(0.0)), axis=1, keepdims=True)
    docs = side[:, EXP_FLIGHT * PIECES].astype(jnp.int32)
    weighted = (partial_value * weight).astype(jnp.bfloat16)

    score_full = lax.all_gather(w_score, "tensor", axis=0, tiled=True) if parts > 1 else w_score
    projected = jnp.sum(weighted.astype(jnp.float32) * score_full[None, :], axis=1)
    hits = (docs[:, None] == jnp.arange(doc_total, dtype=jnp.int32)[None, :]).astype(jnp.float32)
    counts = jnp.sum(hits, axis=0)
    doc_part = jnp.sum(hits * projected[:, None], axis=0)

    pieces = jnp.concatenate(split_wide(doc_part))
    side_out = jnp.zeros((LANES,), jnp.float32).at[: PIECES * doc_total].set(pieces)
    side_out = jnp.broadcast_to(side_out.astype(jnp.bfloat16), (rows, LANES))
    leaving = jnp.concatenate([weighted, side_out], axis=1).reshape(
        members, tok_rows, width + LANES
    )
    returned = lax.all_to_all(leaving, "expert", split_axis=0, concat_axis=0, tiled=True)
    summed = jnp.sum(returned.astype(jnp.float32), axis=0)
    mixed = lax.psum_scatter(summed[:, :width], "tensor", scatter_dimension=1, tiled=True)
    mixed = mixed.astype(jnp.bfloat16)
    totals = summed[0, width : width + PIECES * doc_total].reshape(PIECES, doc_total).sum(axis=0)
    totals = lax.psum(totals, "tensor")
    scores = jax.nn.sigmoid(totals / counts)
    return (mixed, scores)


def solution(mesh):
    in_specs = (
        P(("groups", "expert"), None),
        P(("groups", "expert"), None),
        P(("groups", "expert"), None),
        P(("groups", "expert")),
        P(None, ("expert", "tensor")),
        P(None, ("expert", "tensor")),
        P(("expert", "tensor"), None),
        P("tensor"),
    )
    out_specs = (P(("groups", "expert"), "tensor"), P("groups"))
    return jax.shard_map(local, mesh=mesh, in_specs=in_specs, out_specs=out_specs, check_vma=False)
```

```python
import functools

import jax
import jax.numpy as jnp
from jax import lax
from jax.experimental import pallas as pl
from jax.experimental.pallas import tpu as pltpu
from jax.sharding import PartitionSpec as P

EXP_FLIGHT = 4
LANES = 128
VMEM_LIMIT = 24 * 1024 * 1024
LOAD_FLOPS = 10_000_000


def split_pair(value):
    high = value.astype(jnp.bfloat16).astype(jnp.float32)
    low = (value - high).astype(jnp.bfloat16).astype(jnp.float32)
    return high, low


def call(body, outs, args, in_spaces=None, out_spaces=None, cost=None, scratch=(), limit=VMEM_LIMIT):
    vmem = pltpu.MemorySpace.VMEM
    ins = in_spaces or [vmem] * len(args)
    spaces = out_spaces or [vmem] * len(outs)
    return pl.pallas_call(
        body,
        out_shape=tuple(outs),
        in_specs=[pl.BlockSpec(memory_space=s) for s in ins],
        out_specs=tuple(pl.BlockSpec(memory_space=s) for s in spaces),
        compiler_params=pltpu.CompilerParams(vmem_limit_bytes=limit),
        cost_estimate=cost,
        scratch_shapes=scratch,
    )(*args)


def in_hbm(*arrays):
    return tuple(pltpu.with_memory_space_constraint(a, pltpu.MemorySpace.HBM) for a in arrays)


def pack_body(tokens_ref, ids_ref, gates_ref, docs_ref, out_ref, ids, gates, docs, sems):
    blocks, rows, _ = out_ref.shape
    width = tokens_ref.shape[1]
    small = [
        pltpu.make_async_copy(ids_ref, ids, sems.at[0]),
        pltpu.make_async_copy(gates_ref, gates, sems.at[1]),
        pltpu.make_async_copy(docs_ref, docs, sems.at[2]),
    ]
    large = [
        pltpu.make_async_copy(tokens_ref, out_ref.at[b, :, pl.ds(0, width)], sems.at[3 + b])
        for b in range(blocks)
    ]
    for copy in small + large:
        copy.start()
    for copy in small:
        copy.wait()
    lane = lax.broadcasted_iota(jnp.int32, (rows, LANES), 1)
    row = lax.broadcasted_iota(jnp.int32, (rows, LANES), 0)
    weight = jnp.zeros((rows, LANES), jnp.float32)
    doc = jnp.zeros((rows, LANES), jnp.float32)
    for r in range(rows):
        for k in range(ids.shape[1]):
            named = ids[r, k]
            hit = (row == r) & ((lane == named) | (lane == named + EXP_FLIGHT))
            weight = jnp.where(hit, gates[r, k], weight)
        doc = jnp.where(row == r, docs[r].astype(jnp.float32), doc)
    high, low = split_pair(weight)
    side = jnp.where(lane < EXP_FLIGHT, high, low)
    side = jnp.where(lane == 2 * EXP_FLIGHT, doc, side).astype(jnp.bfloat16)
    for b in range(blocks):
        out_ref[b, :, width:] = side
    for copy in large:
        copy.wait()


def load_body(*refs):
    count = (len(refs) - 1) // 2
    sems = refs[-1]
    copies = [
        pltpu.make_async_copy(refs[i], refs[count + i], sems.at[i]) for i in range(count)
    ]
    for copy in copies:
        copy.start()
    for copy in copies:
        copy.wait()


def expert_rows(spread, block, w_gate_ref, w_up_ref, w_down_ref, w_score_ref):
    blocks, each, total = block.shape
    rows = blocks * each
    width = total - LANES
    flat = block.reshape(rows, total)
    held = flat[:, :width]
    side = flat[:, width:].astype(jnp.float32)
    gate = jnp.dot(held, w_gate_ref[...], preferred_element_type=jnp.float32)
    up = jnp.dot(held, w_up_ref[...], preferred_element_type=jnp.float32)
    hidden = (gate / (1.0 + jnp.exp(-gate)) * up).astype(jnp.bfloat16)
    part = jnp.dot(hidden, w_down_ref[...], preferred_element_type=jnp.float32)
    own = lax.axis_index("expert") // spread
    lane = lax.broadcasted_iota(jnp.int32, (rows, LANES), 1)
    mine = (lane == own) | (lane == own + EXP_FLIGHT)
    weight = jnp.sum(jnp.where(mine, side, 0.0), axis=1, keepdims=True)
    doc = jnp.sum(jnp.where(lane == 2 * EXP_FLIGHT, side, 0.0), axis=1, keepdims=True)
    part = part * weight
    projected = jnp.sum(part * w_score_ref[...], axis=1, keepdims=True)
    hits = doc == lane.astype(jnp.float32)
    sums = jnp.sum(jnp.where(hits, projected, 0.0), axis=0, keepdims=True)
    counts = jnp.sum(jnp.where(hits, 1.0, 0.0), axis=0, keepdims=True)
    return part, sums, counts


def side_rows(sums, rows):
    row = lax.broadcasted_iota(jnp.int32, (rows, LANES), 0)
    high, low = split_pair(sums)
    side = jnp.where(row == 0, high, jnp.where(row == 1, low, 0.0))
    return side.astype(jnp.bfloat16)


def first_body(spread, x_ref, w_gate_ref, w_up_ref, w_down_ref, w_score_ref, part_ref, stat_ref):
    part, sums, counts = expert_rows(
        spread, x_ref[...], w_gate_ref, w_up_ref, w_down_ref, w_score_ref
    )
    part_ref[...] = part
    stat_ref[0:1] = sums
    stat_ref[1:2] = counts


def second_body(
    spread, x_ref, w_gate_ref, w_up_ref, w_down_ref, w_score_ref, before_ref, out_ref, stat_ref
):
    blocks, each, total = x_ref.shape
    width = total - LANES
    part, sums, counts = expert_rows(
        spread, x_ref[...], w_gate_ref, w_up_ref, w_down_ref, w_score_ref
    )
    sums = sums + before_ref[0:1]
    stat_ref[0:1] = sums
    stat_ref[1:2] = counts + before_ref[1:2]
    out_ref[:, :, :width] = part.astype(jnp.bfloat16).reshape(blocks, each, width)
    side = side_rows(sums, each)
    for b in range(blocks):
        out_ref[b, :, width:] = side


def add_body(part_ref, came_ref, stat_ref, out_ref):
    blocks, each, total = came_ref.shape
    width = total - LANES
    came = came_ref[...].reshape(blocks * each, total)
    added = part_ref[...] + came[:, :width].astype(jnp.float32)
    out_ref[:, :, :width] = added.astype(jnp.bfloat16).reshape(blocks, each, width)
    other = jnp.sum(came[:each, width:].astype(jnp.float32), axis=0, keepdims=True)
    side = side_rows(stat_ref[0:1] + other, each)
    for b in range(blocks):
        out_ref[b, :, width:] = side


def last_body(came_ref, stat_ref, mixed_ref, scores_ref):
    blocks, each, total = came_ref.shape
    width = total - LANES
    summed = came_ref[0].astype(jnp.float32)
    for b in range(1, blocks):
        summed = summed + came_ref[b].astype(jnp.float32)
    mixed_ref[...] = summed[:, :width].astype(jnp.bfloat16)
    totals = jnp.sum(summed[:, width:], axis=0, keepdims=True)
    ratio = totals / stat_ref[1:2]
    scores = 1.0 / (1.0 + jnp.exp(-ratio))
    lane = lax.broadcasted_iota(jnp.int32, (1, LANES), 1)
    for d in range(scores_ref.shape[0]):
        scores_ref[d] = jnp.sum(jnp.where(lane == d, scores, 0.0))


def local(tokens, expert_ids, gate_weights, doc_ids, w_gate, w_up, w_down, w_score):
    members = lax.axis_size("expert")
    parts = lax.axis_size("tensor")
    tok_rows, width = tokens.shape
    rows = members * tok_rows
    spread = members // EXP_FLIGHT
    doc_total = rows // 8
    half = members // 2
    total = width + LANES
    vmem, smem = pltpu.MemorySpace.VMEM, pltpu.MemorySpace.SMEM
    alike = [list(range(side, members, 2)) for side in range(2)]
    swap = [(i, i ^ 1) for i in range(members)]
    exchange = functools.partial(
        lax.all_to_all, axis_name="expert", split_axis=0, concat_axis=0, axis_index_groups=alike, tiled=True
    )
    packet = jax.ShapeDtypeStruct((half, tok_rows, total), jnp.bfloat16)
    stat = jax.ShapeDtypeStruct((2, LANES), jnp.float32)

    hbm = pltpu.MemorySpace.HBM

    (outgoing,) = call(
        pack_body,
        [packet],
        in_hbm(tokens, expert_ids, gate_weights, doc_ids),
        [hbm] * 4,
        scratch=(
            pltpu.SMEM(expert_ids.shape, jnp.int32),
            pltpu.SMEM(gate_weights.shape, jnp.float32),
            pltpu.SMEM(doc_ids.shape, jnp.int32),
            pltpu.SemaphoreType.DMA((3 + half,)),
        ),
    )
    score_full = lax.all_gather(w_score, "tensor", axis=0, tiled=True) if parts > 1 else w_score
    weights = (w_gate, w_up, w_down, score_full.reshape(1, -1))
    near = exchange(outgoing)
    size = sum(w.size * w.dtype.itemsize for w in weights)
    weights = call(
        load_body,
        [jax.ShapeDtypeStruct(w.shape, w.dtype) for w in weights],
        in_hbm(*weights),
        [hbm] * len(weights),
        cost=pl.CostEstimate(flops=LOAD_FLOPS, bytes_accessed=2 * size, transcendentals=0),
        scratch=(pltpu.SemaphoreType.DMA((len(weights),)),),
    )
    near, *weights = lax.optimization_barrier((near, *weights))
    far = lax.ppermute(near, "expert", swap)
    kept, stat_near = call(
        functools.partial(first_body, spread),
        [jax.ShapeDtypeStruct((rows // 2, width), jnp.float32), stat],
        (near, *weights),
    )
    leaving, stat_all = call(
        functools.partial(second_body, spread), [packet, stat], (far, *weights, stat_near)
    )
    came = lax.ppermute(leaving, "expert", swap)
    (sending,) = call(add_body, [packet], (kept, came, stat_all))
    returned = exchange(sending)
    if parts == 1:
        return call(
            last_body,
            [
                jax.ShapeDtypeStruct((tok_rows, width), jnp.bfloat16),
                jax.ShapeDtypeStruct((doc_total,), jnp.float32),
            ],
            (returned, stat_all),
            None,
            [vmem, smem],
        )
    summed = jnp.sum(returned.astype(jnp.float32), axis=0)
    mixed = lax.psum_scatter(summed[:, :width], "tensor", scatter_dimension=1, tiled=True)
    totals = lax.psum(jnp.sum(summed[:, width : width + doc_total], axis=0), "tensor")
    scores = jax.nn.sigmoid(totals / stat_all[1, :doc_total])
    return (mixed.astype(jnp.bfloat16), scores)


def solution(mesh):
    in_specs = (
        P(("groups", "expert"), None),
        P(("groups", "expert"), None),
        P(("groups", "expert"), None),
        P(("groups", "expert")),
        P(None, ("expert", "tensor")),
        P(None, ("expert", "tensor")),
        P(("expert", "tensor"), None),
        P("tensor"),
    )
    out_specs = (P(("groups", "expert"), "tensor"), P("groups"))
    return jax.shard_map(local, mesh=mesh, in_specs=in_specs, out_specs=out_specs, check_vma=False)
```

```python
import functools

import jax
import jax.numpy as jnp
from jax import lax
from jax.experimental import pallas as pl
from jax.experimental.pallas import tpu as pltpu
from jax.sharding import PartitionSpec as P

EXP_FLIGHT = 4
LANES = 128
VMEM_LIMIT = 24 * 1024 * 1024
PACK_FLOPS = 10**10
PACK_BYTES = 3 * 10**7


def split_pair(value):
    high = value.astype(jnp.bfloat16).astype(jnp.float32)
    low = (value - high).astype(jnp.bfloat16).astype(jnp.float32)
    return high, low


def call(body, outs, args, in_spaces=None, out_spaces=None, cost=None, scratch=(), limit=VMEM_LIMIT):
    vmem = pltpu.MemorySpace.VMEM
    ins = in_spaces or [vmem] * len(args)
    spaces = out_spaces or [vmem] * len(outs)
    return pl.pallas_call(
        body,
        out_shape=tuple(outs),
        in_specs=[pl.BlockSpec(memory_space=s) for s in ins],
        out_specs=tuple(pl.BlockSpec(memory_space=s) for s in spaces),
        compiler_params=pltpu.CompilerParams(vmem_limit_bytes=limit),
        cost_estimate=cost,
        scratch_shapes=scratch,
    )(*args)


def in_hbm(*arrays):
    return tuple(pltpu.with_memory_space_constraint(a, pltpu.MemorySpace.HBM) for a in arrays)


def pack_body(tokens_ref, ids_ref, gates_ref, docs_ref, out_ref, ids, gates, docs, sems):
    blocks, rows, _ = out_ref.shape
    width = tokens_ref.shape[1]
    small = [
        pltpu.make_async_copy(ids_ref, ids, sems.at[0]),
        pltpu.make_async_copy(gates_ref, gates, sems.at[1]),
        pltpu.make_async_copy(docs_ref, docs, sems.at[2]),
    ]
    large = [
        pltpu.make_async_copy(tokens_ref, out_ref.at[b, :, pl.ds(0, width)], sems.at[3 + b])
        for b in range(blocks)
    ]
    for copy in small + large:
        copy.start()
    for copy in small:
        copy.wait()
    lane = lax.broadcasted_iota(jnp.int32, (rows, LANES), 1)
    row = lax.broadcasted_iota(jnp.int32, (rows, LANES), 0)
    weight = jnp.zeros((rows, LANES), jnp.float32)
    doc = jnp.zeros((rows, LANES), jnp.float32)
    for r in range(rows):
        for k in range(ids.shape[1]):
            named = ids[r, k]
            hit = (row == r) & ((lane == named) | (lane == named + EXP_FLIGHT))
            weight = jnp.where(hit, gates[r, k], weight)
        doc = jnp.where(row == r, docs[r].astype(jnp.float32), doc)
    high, low = split_pair(weight)
    side = jnp.where(lane < EXP_FLIGHT, high, low)
    side = jnp.where(lane == 2 * EXP_FLIGHT, doc, side).astype(jnp.bfloat16)
    for b in range(blocks):
        out_ref[b, :, width:] = side
    for copy in large:
        copy.wait()


def expert_rows(spread, block, w_gate_ref, w_up_ref, w_down_ref, w_score_ref):
    blocks, each, total = block.shape
    rows = blocks * each
    width = total - LANES
    flat = block.reshape(rows, total)
    held = flat[:, :width]
    side = flat[:, width:].astype(jnp.float32)
    gate = jnp.dot(held, w_gate_ref[...], preferred_element_type=jnp.float32)
    up = jnp.dot(held, w_up_ref[...], preferred_element_type=jnp.float32)
    hidden = (gate / (1.0 + jnp.exp(-gate)) * up).astype(jnp.bfloat16)
    part = jnp.dot(hidden, w_down_ref[...], preferred_element_type=jnp.float32)
    own = lax.axis_index("expert") // spread
    lane = lax.broadcasted_iota(jnp.int32, (rows, LANES), 1)
    mine = (lane == own) | (lane == own + EXP_FLIGHT)
    weight = jnp.sum(jnp.where(mine, side, 0.0), axis=1, keepdims=True)
    doc = jnp.sum(jnp.where(lane == 2 * EXP_FLIGHT, side, 0.0), axis=1, keepdims=True)
    part = part * weight
    projected = jnp.sum(part * w_score_ref[...], axis=1, keepdims=True)
    hits = doc == lane.astype(jnp.float32)
    sums = jnp.sum(jnp.where(hits, projected, 0.0), axis=0, keepdims=True)
    counts = jnp.sum(jnp.where(hits, 1.0, 0.0), axis=0, keepdims=True)
    return part, sums, counts


def side_rows(sums, rows):
    row = lax.broadcasted_iota(jnp.int32, (rows, LANES), 0)
    high, low = split_pair(sums)
    side = jnp.where(row == 0, high, jnp.where(row == 1, low, 0.0))
    return side.astype(jnp.bfloat16)


def first_body(spread, x_ref, w_gate_ref, w_up_ref, w_down_ref, w_score_ref, part_ref, stat_ref):
    part, sums, counts = expert_rows(
        spread, x_ref[...], w_gate_ref, w_up_ref, w_down_ref, w_score_ref
    )
    part_ref[...] = part
    stat_ref[0:1] = sums
    stat_ref[1:2] = counts


def second_body(
    spread, x_ref, w_gate_ref, w_up_ref, w_down_ref, w_score_ref, before_ref, out_ref, stat_ref
):
    blocks, each, total = x_ref.shape
    width = total - LANES
    part, sums, counts = expert_rows(
        spread, x_ref[...], w_gate_ref, w_up_ref, w_down_ref, w_score_ref
    )
    sums = sums + before_ref[0:1]
    stat_ref[0:1] = sums
    stat_ref[1:2] = counts + before_ref[1:2]
    out_ref[:, :, :width] = part.astype(jnp.bfloat16).reshape(blocks, each, width)
    side = side_rows(sums, each)
    for b in range(blocks):
        out_ref[b, :, width:] = side


def add_body(part_ref, came_ref, stat_ref, out_ref):
    blocks, each, total = came_ref.shape
    width = total - LANES
    came = came_ref[...].reshape(blocks * each, total)
    added = part_ref[...] + came[:, :width].astype(jnp.float32)
    out_ref[:, :, :width] = added.astype(jnp.bfloat16).reshape(blocks, each, width)
    other = jnp.sum(came[:each, width:].astype(jnp.float32), axis=0, keepdims=True)
    side = side_rows(stat_ref[0:1] + other, each)
    for b in range(blocks):
        out_ref[b, :, width:] = side


def last_body(came_ref, stat_ref, mixed_ref, scores_ref):
    blocks, each, total = came_ref.shape
    width = total - LANES
    summed = came_ref[0].astype(jnp.float32)
    for b in range(1, blocks):
        summed = summed + came_ref[b].astype(jnp.float32)
    mixed_ref[...] = summed[:, :width].astype(jnp.bfloat16)
    totals = jnp.sum(summed[:, width:], axis=0, keepdims=True)
    ratio = totals / stat_ref[1:2]
    scores = 1.0 / (1.0 + jnp.exp(-ratio))
    lane = lax.broadcasted_iota(jnp.int32, (1, LANES), 1)
    for d in range(scores_ref.shape[0]):
        scores_ref[d] = jnp.sum(jnp.where(lane == d, scores, 0.0))


def local(tokens, expert_ids, gate_weights, doc_ids, w_gate, w_up, w_down, w_score):
    members = lax.axis_size("expert")
    parts = lax.axis_size("tensor")
    tok_rows, width = tokens.shape
    rows = members * tok_rows
    spread = members // EXP_FLIGHT
    doc_total = rows // 8
    half = members // 2
    total = width + LANES
    vmem, smem = pltpu.MemorySpace.VMEM, pltpu.MemorySpace.SMEM
    pairs = list(range(half))
    alike = []
    for side in range(2):
        root = half // 2 + (1 - side) % half
        order = [root] + [q for q in pairs if q != root]
        alike.append([2 * q + (q + side) % 2 for q in order])
    swap = [(i, i ^ 1) for i in range(members)]
    exchange = functools.partial(
        lax.all_to_all, axis_name="expert", split_axis=0, concat_axis=0, axis_index_groups=alike, tiled=True
    )
    packet = jax.ShapeDtypeStruct((half, tok_rows, total), jnp.bfloat16)
    stat = jax.ShapeDtypeStruct((2, LANES), jnp.float32)

    hbm = pltpu.MemorySpace.HBM

    (outgoing,) = call(
        pack_body,
        [packet],
        in_hbm(tokens, expert_ids, gate_weights, doc_ids),
        [hbm] * 4,
        scratch=(
            pltpu.SMEM(expert_ids.shape, jnp.int32),
            pltpu.SMEM(gate_weights.shape, jnp.float32),
            pltpu.SMEM(doc_ids.shape, jnp.int32),
            pltpu.SemaphoreType.DMA((3 + half,)),
        ),
        cost=pl.CostEstimate(flops=PACK_FLOPS, bytes_accessed=PACK_BYTES, transcendentals=0),
    )
    score_full = lax.all_gather(w_score, "tensor", axis=0, tiled=True) if parts > 1 else w_score
    weights = (w_gate, w_up, w_down, score_full.reshape(1, -1))
    near = exchange(outgoing)
    flops = 3 * 2 * rows // 2 * width * w_gate.shape[1]
    size = sum(w.size * w.dtype.itemsize for w in weights)
    cost = pl.CostEstimate(flops=flops, bytes_accessed=size + rows * width * 4, transcendentals=0)
    far = lax.ppermute(near, "expert", swap)
    kept, stat_near = call(
        functools.partial(first_body, spread),
        [jax.ShapeDtypeStruct((rows // 2, width), jnp.float32), stat],
        (near, *weights),
        cost=cost,
    )
    leaving, stat_all = call(
        functools.partial(second_body, spread), [packet, stat], (far, *weights, stat_near), cost=cost
    )
    came = lax.ppermute(leaving, "expert", swap)
    (sending,) = call(add_body, [packet], (kept, came, stat_all))
    returned = exchange(sending)
    if parts == 1:
        return call(
            last_body,
            [
                jax.ShapeDtypeStruct((tok_rows, width), jnp.bfloat16),
                jax.ShapeDtypeStruct((doc_total,), jnp.float32),
            ],
            (returned, stat_all),
            None,
            [vmem, smem],
        )
    summed = jnp.sum(returned.astype(jnp.float32), axis=0)
    mixed = lax.psum_scatter(summed[:, :width], "tensor", scatter_dimension=1, tiled=True)
    totals = lax.psum(jnp.sum(summed[:, width : width + doc_total], axis=0), "tensor")
    scores = jax.nn.sigmoid(totals / stat_all[1, :doc_total])
    return (mixed.astype(jnp.bfloat16), scores)


def solution(mesh):
    in_specs = (
        P(("groups", "expert"), None),
        P(("groups", "expert"), None),
        P(("groups", "expert"), None),
        P(("groups", "expert")),
        P(None, ("expert", "tensor")),
        P(None, ("expert", "tensor")),
        P(("expert", "tensor"), None),
        P("tensor"),
    )
    out_specs = (P(("groups", "expert"), "tensor"), P("groups"))
    return jax.shard_map(local, mesh=mesh, in_specs=in_specs, out_specs=out_specs, check_vma=False)
```

```python
import functools

import jax
import jax.numpy as jnp
from jax import lax
from jax.experimental import pallas as pl
from jax.experimental.pallas import tpu as pltpu
from jax.sharding import PartitionSpec as P

EXP_FLIGHT = 4
LANES = 128
VMEM_LIMIT = 24 * 1024 * 1024
PACK_FLOPS = 10**10
PACK_BYTES = 3 * 10**7


def split_pair(value):
    high = value.astype(jnp.bfloat16).astype(jnp.float32)
    low = (value - high).astype(jnp.bfloat16).astype(jnp.float32)
    return high, low


def call(body, outs, args, in_spaces=None, out_spaces=None, cost=None, scratch=(), limit=VMEM_LIMIT):
    vmem = pltpu.MemorySpace.VMEM
    ins = in_spaces or [vmem] * len(args)
    spaces = out_spaces or [vmem] * len(outs)
    return pl.pallas_call(
        body,
        out_shape=tuple(outs),
        in_specs=[pl.BlockSpec(memory_space=s) for s in ins],
        out_specs=tuple(pl.BlockSpec(memory_space=s) for s in spaces),
        compiler_params=pltpu.CompilerParams(vmem_limit_bytes=limit),
        cost_estimate=cost,
        scratch_shapes=scratch,
    )(*args)


def exchange_groups(half):
    middle = half // 2
    exchanges = []
    for roots in ((middle + 1, middle + 1), (middle + 1, middle)):
        groups = []
        for side, root in enumerate(roots):
            order = [root] + [q for q in range(half) if q != root]
            groups.append([2 * q + (int(q >= middle) ^ side) for q in order])
        exchanges.append(groups)
    return exchanges


def in_hbm(*arrays):
    return tuple(pltpu.with_memory_space_constraint(a, pltpu.MemorySpace.HBM) for a in arrays)


def pack_body(tokens_ref, ids_ref, gates_ref, docs_ref, out_ref, ids, gates, docs, held, sems):
    blocks, rows, _ = out_ref.shape
    width = tokens_ref.shape[1]
    copies = [
        pltpu.make_async_copy(ids_ref, ids, sems.at[0]),
        pltpu.make_async_copy(gates_ref, gates, sems.at[1]),
        pltpu.make_async_copy(docs_ref, docs, sems.at[2]),
        pltpu.make_async_copy(tokens_ref, held, sems.at[3]),
    ]
    for copy in copies:
        copy.start()
    for copy in copies[:3]:
        copy.wait()
    lane = lax.broadcasted_iota(jnp.int32, (rows, LANES), 1)
    row = lax.broadcasted_iota(jnp.int32, (rows, LANES), 0)
    weight = jnp.zeros((rows, LANES), jnp.float32)
    doc = jnp.zeros((rows, LANES), jnp.float32)
    for r in range(rows):
        for k in range(ids.shape[1]):
            named = ids[r, k]
            hit = (row == r) & ((lane == named) | (lane == named + EXP_FLIGHT))
            weight = jnp.where(hit, gates[r, k], weight)
        doc = jnp.where(row == r, docs[r].astype(jnp.float32), doc)
    high, low = split_pair(weight)
    side = jnp.where(lane < EXP_FLIGHT, high, low)
    side = jnp.where(lane == 2 * EXP_FLIGHT, doc, side).astype(jnp.bfloat16)
    for b in range(blocks):
        out_ref[b, :, width:] = side
    copies[3].wait()
    block = held[...]
    for b in range(blocks):
        out_ref[b, :, :width] = block


def expert_rows(spread, block, w_gate_ref, w_up_ref, w_down_ref, w_score_ref):
    blocks, each, total = block.shape
    rows = blocks * each
    width = total - LANES
    flat = block.reshape(rows, total)
    held = flat[:, :width]
    side = flat[:, width:].astype(jnp.float32)
    gate = jnp.dot(held, w_gate_ref[...], preferred_element_type=jnp.float32)
    up = jnp.dot(held, w_up_ref[...], preferred_element_type=jnp.float32)
    hidden = (gate / (1.0 + jnp.exp(-gate)) * up).astype(jnp.bfloat16)
    part = jnp.dot(hidden, w_down_ref[...], preferred_element_type=jnp.float32)
    own = lax.axis_index("expert") // spread
    lane = lax.broadcasted_iota(jnp.int32, (rows, LANES), 1)
    mine = (lane == own) | (lane == own + EXP_FLIGHT)
    weight = jnp.sum(jnp.where(mine, side, 0.0), axis=1, keepdims=True)
    doc = jnp.sum(jnp.where(lane == 2 * EXP_FLIGHT, side, 0.0), axis=1, keepdims=True)
    part = part * weight
    projected = jnp.sum(part * w_score_ref[...], axis=1, keepdims=True)
    hits = doc == lane.astype(jnp.float32)
    sums = jnp.sum(jnp.where(hits, projected, 0.0), axis=0, keepdims=True)
    counts = jnp.sum(jnp.where(hits, 1.0, 0.0), axis=0, keepdims=True)
    return part, sums, counts


def side_rows(sums, rows):
    row = lax.broadcasted_iota(jnp.int32, (rows, LANES), 0)
    high, low = split_pair(sums)
    side = jnp.where(row == 0, high, jnp.where(row == 1, low, 0.0))
    return side.astype(jnp.bfloat16)


def first_body(spread, x_ref, w_gate_ref, w_up_ref, w_down_ref, w_score_ref, part_ref, stat_ref):
    part, sums, counts = expert_rows(
        spread, x_ref[...], w_gate_ref, w_up_ref, w_down_ref, w_score_ref
    )
    part_ref[...] = part
    stat_ref[0:1] = sums
    stat_ref[1:2] = counts


def second_body(
    spread, x_ref, w_gate_ref, w_up_ref, w_down_ref, w_score_ref, before_ref, out_ref, stat_ref
):
    blocks, each, total = x_ref.shape
    width = total - LANES
    part, sums, counts = expert_rows(
        spread, x_ref[...], w_gate_ref, w_up_ref, w_down_ref, w_score_ref
    )
    sums = sums + before_ref[0:1]
    stat_ref[0:1] = sums
    stat_ref[1:2] = counts + before_ref[1:2]
    out_ref[:, :, :width] = part.astype(jnp.bfloat16).reshape(blocks, each, width)
    side = side_rows(sums, each)
    for b in range(blocks):
        out_ref[b, :, width:] = side


def add_body(moves, part_ref, came_ref, stat_ref, out_ref):
    blocks, each, total = came_ref.shape
    width = total - LANES
    came = came_ref[...].reshape(blocks * each, total)
    added = part_ref[...] + came[:, :width].astype(jnp.float32)
    added = added.astype(jnp.bfloat16).reshape(blocks, each, width)
    me = lax.axis_index("expert")
    side = (me + me // blocks) % 2
    for b in range(blocks):
        to = moves[0][b] if moves[0][b] == moves[1][b] else jnp.where(side == 0, moves[0][b], moves[1][b])
        out_ref[to, :, :width] = added[b]
    other = jnp.sum(came[:each, width:].astype(jnp.float32), axis=0, keepdims=True)
    side = side_rows(stat_ref[0:1] + other, each)
    for b in range(blocks):
        out_ref[b, :, width:] = side


def last_body(came_ref, stat_ref, mixed_ref, scores_ref):
    blocks, each, total = came_ref.shape
    width = total - LANES
    summed = came_ref[0].astype(jnp.float32)
    for b in range(1, blocks):
        summed = summed + came_ref[b].astype(jnp.float32)
    mixed_ref[...] = summed[:, :width].astype(jnp.bfloat16)
    totals = jnp.sum(summed[:, width:], axis=0, keepdims=True)
    ratio = totals / stat_ref[1:2]
    scores = 1.0 / (1.0 + jnp.exp(-ratio))
    lane = lax.broadcasted_iota(jnp.int32, (1, LANES), 1)
    for d in range(scores_ref.shape[0]):
        scores_ref[d] = jnp.sum(jnp.where(lane == d, scores, 0.0))


def local(tokens, expert_ids, gate_weights, doc_ids, w_gate, w_up, w_down, w_score):
    members = lax.axis_size("expert")
    parts = lax.axis_size("tensor")
    tok_rows, width = tokens.shape
    rows = members * tok_rows
    spread = members // EXP_FLIGHT
    doc_total = rows // 8
    half = members // 2
    total = width + LANES
    vmem, smem = pltpu.MemorySpace.VMEM, pltpu.MemorySpace.SMEM
    first_groups, second_groups = exchange_groups(half)
    moves = [[b.index(m) for m in a] for a, b in zip(first_groups, second_groups)]
    swap = [(i, i ^ 1) for i in range(members)]
    exchange = functools.partial(
        lax.all_to_all, axis_name="expert", split_axis=0, concat_axis=0, tiled=True
    )
    packet = jax.ShapeDtypeStruct((half, tok_rows, total), jnp.bfloat16)
    stat = jax.ShapeDtypeStruct((2, LANES), jnp.float32)

    hbm = pltpu.MemorySpace.HBM

    (outgoing,) = call(
        pack_body,
        [packet],
        in_hbm(tokens, expert_ids, gate_weights, doc_ids),
        [hbm] * 4,
        scratch=(
            pltpu.SMEM(expert_ids.shape, jnp.int32),
            pltpu.SMEM(gate_weights.shape, jnp.float32),
            pltpu.SMEM(doc_ids.shape, jnp.int32),
            pltpu.VMEM(tokens.shape, tokens.dtype),
            pltpu.SemaphoreType.DMA((4,)),
        ),
        cost=pl.CostEstimate(flops=PACK_FLOPS, bytes_accessed=PACK_BYTES, transcendentals=0),
    )
    score_full = lax.all_gather(w_score, "tensor", axis=0, tiled=True) if parts > 1 else w_score
    weights = (w_gate, w_up, w_down, score_full.reshape(1, -1))
    near = exchange(outgoing, axis_index_groups=first_groups)
    flops = 3 * 2 * rows // 2 * width * w_gate.shape[1]
    size = sum(w.size * w.dtype.itemsize for w in weights)
    cost = pl.CostEstimate(flops=flops, bytes_accessed=size + rows * width * 4, transcendentals=0)
    far = lax.ppermute(near, "expert", swap)
    kept, stat_near = call(
        functools.partial(first_body, spread),
        [jax.ShapeDtypeStruct((rows // 2, width), jnp.float32), stat],
        (near, *weights),
        cost=cost,
    )
    leaving, stat_all = call(
        functools.partial(second_body, spread), [packet, stat], (far, *weights, stat_near), cost=cost
    )
    came = lax.ppermute(leaving, "expert", swap)
    (sending,) = call(functools.partial(add_body, moves), [packet], (kept, came, stat_all))
    returned = exchange(sending, axis_index_groups=second_groups)
    if parts == 1:
        return call(
            last_body,
            [
                jax.ShapeDtypeStruct((tok_rows, width), jnp.bfloat16),
                jax.ShapeDtypeStruct((doc_total,), jnp.float32),
            ],
            (returned, stat_all),
            None,
            [vmem, smem],
        )
    summed = jnp.sum(returned.astype(jnp.float32), axis=0)
    mixed = lax.psum_scatter(summed[:, :width], "tensor", scatter_dimension=1, tiled=True)
    totals = lax.psum(jnp.sum(summed[:, width : width + doc_total], axis=0), "tensor")
    scores = jax.nn.sigmoid(totals / stat_all[1, :doc_total])
    return (mixed.astype(jnp.bfloat16), scores)


def solution(mesh):
    in_specs = (
        P(("groups", "expert"), None),
        P(("groups", "expert"), None),
        P(("groups", "expert"), None),
        P(("groups", "expert")),
        P(None, ("expert", "tensor")),
        P(None, ("expert", "tensor")),
        P(("expert", "tensor"), None),
        P("tensor"),
    )
    out_specs = (P(("groups", "expert"), "tensor"), P("groups"))
    return jax.shard_map(local, mesh=mesh, in_specs=in_specs, out_specs=out_specs, check_vma=False)
```

```python
import functools

import jax
import jax.numpy as jnp
from jax import lax
from jax.experimental import pallas as pl
from jax.experimental.pallas import tpu as pltpu
from jax.sharding import PartitionSpec as P

EXP_FLIGHT = 4
LANES = 128
VMEM_LIMIT = 24 * 1024 * 1024
PACK_FLOPS = 10**10
PACK_BYTES = 3 * 10**7


def split_pair(value):
    high = value.astype(jnp.bfloat16).astype(jnp.float32)
    low = (value - high).astype(jnp.bfloat16).astype(jnp.float32)
    return high, low


def call(body, outs, args, in_spaces=None, out_spaces=None, cost=None, scratch=(), limit=VMEM_LIMIT):
    vmem = pltpu.MemorySpace.VMEM
    ins = in_spaces or [vmem] * len(args)
    spaces = out_spaces or [vmem] * len(outs)
    return pl.pallas_call(
        body,
        out_shape=tuple(outs),
        in_specs=[pl.BlockSpec(memory_space=s) for s in ins],
        out_specs=tuple(pl.BlockSpec(memory_space=s) for s in spaces),
        compiler_params=pltpu.CompilerParams(vmem_limit_bytes=limit),
        cost_estimate=cost,
        scratch_shapes=scratch,
    )(*args)


def exchange_groups(half):
    middle = half // 2
    exchanges = []
    for roots in ((middle + 1, middle + 1), (middle + 1, middle)):
        groups = []
        for side, root in enumerate(roots):
            order = [root] + [q for q in range(half) if q != root]
            groups.append([2 * q + (int(q >= middle) ^ side) for q in order])
        exchanges.append(groups)
    return exchanges


def in_hbm(*arrays):
    return tuple(pltpu.with_memory_space_constraint(a, pltpu.MemorySpace.HBM) for a in arrays)


def pack_body(tokens_ref, ids_ref, gates_ref, docs_ref, out_ref, ids, gates, docs, held, sems):
    blocks, rows, _ = out_ref.shape
    width = tokens_ref.shape[1]
    copies = [
        pltpu.make_async_copy(ids_ref, ids, sems.at[0]),
        pltpu.make_async_copy(gates_ref, gates, sems.at[1]),
        pltpu.make_async_copy(docs_ref, docs, sems.at[2]),
        pltpu.make_async_copy(tokens_ref, held, sems.at[3]),
    ]
    for copy in copies:
        copy.start()
    copies[3].wait()
    block = held[...]
    for b in range(blocks):
        out_ref[b, :, :width] = block
    for copy in copies[:3]:
        copy.wait()
    lane = lax.broadcasted_iota(jnp.int32, (rows, LANES), 1)
    row = lax.broadcasted_iota(jnp.int32, (rows, LANES), 0)
    weight = jnp.zeros((rows, LANES), jnp.float32)
    doc = jnp.zeros((rows, LANES), jnp.float32)
    for r in range(rows):
        for k in range(ids.shape[1]):
            named = ids[r, k]
            hit = (row == r) & ((lane == named) | (lane == named + EXP_FLIGHT))
            weight = jnp.where(hit, gates[r, k], weight)
        doc = jnp.where(row == r, docs[r].astype(jnp.float32), doc)
    high, low = split_pair(weight)
    side = jnp.where(lane < EXP_FLIGHT, high, low)
    side = jnp.where(lane == 2 * EXP_FLIGHT, doc, side).astype(jnp.bfloat16)
    for b in range(blocks):
        out_ref[b, :, width:] = side


def hidden_rows(held, w_gate, w_up):
    gate = jnp.dot(held, w_gate, preferred_element_type=jnp.float32)
    up = jnp.dot(held, w_up, preferred_element_type=jnp.float32)
    return (gate / (1.0 + jnp.exp(-gate)) * up).astype(jnp.bfloat16)


def score_rows(w_down, score):
    row = lax.broadcasted_iota(jnp.int32, (8, score.shape[1]), 0)
    pieces = jnp.zeros((8, score.shape[1]), jnp.float32)
    rest = score
    for i in range(3):
        piece = rest.astype(jnp.bfloat16).astype(jnp.float32)
        pieces = jnp.where(row == i, piece, pieces)
        rest = rest - piece
    added = lax.dot_general(
        pieces.astype(jnp.bfloat16), w_down, (((1,), (1,)), ((), ())), preferred_element_type=jnp.float32
    )
    return jnp.sum(added, axis=0, keepdims=True)


def hidden_body(spread, doc_total, x_ref, *refs):
    gates, ups = refs[0:2], refs[2:4]
    hidden_ref, weight_ref, stat_ref = refs[4:]
    blocks, each, total = x_ref.shape
    rows = blocks * each
    width = total - LANES
    flat = x_ref[...].reshape(rows, total)
    held = flat[:, :width]
    side = flat[:, width:].astype(jnp.float32)
    own = lax.axis_index("expert") // spread
    lane = lax.broadcasted_iota(jnp.int32, (rows, LANES), 1)
    mine = (lane == own) | (lane == own + EXP_FLIGHT)
    weight = jnp.sum(jnp.where(mine, side, 0.0), axis=1, keepdims=True)
    doc = jnp.sum(jnp.where(lane == 2 * EXP_FLIGHT, side, 0.0), axis=1, keepdims=True)
    weight_ref[...] = jnp.broadcast_to(weight, (rows, LANES))
    stat_ref[...] = jnp.zeros(stat_ref.shape, jnp.float32)
    hits = jnp.where(doc == lane.astype(jnp.float32), 1.0, 0.0)
    stat_ref[doc_total : doc_total + 1, :LANES] = jnp.sum(hits, axis=0, keepdims=True)
    units = gates[0].shape[1]
    for i in range(2):
        hidden = hidden_rows(held, gates[i][...], ups[i][...])
        hidden_ref[:, i * units : (i + 1) * units] = hidden
        hidden = hidden.astype(jnp.float32) * weight
        for d in range(doc_total):
            chosen = jnp.where(doc == float(d), hidden, 0.0)
            stat_ref[d : d + 1, i * units : (i + 1) * units] = jnp.sum(chosen, axis=0, keepdims=True)


def down_body(hidden_ref, weight_ref, own_ref, other_ref, score_ref, out_ref, reach_ref):
    units = own_ref.shape[0]
    part = jnp.dot(hidden_ref[:, :units], own_ref[...], preferred_element_type=jnp.float32)
    part += jnp.dot(hidden_ref[:, units:], other_ref[...], preferred_element_type=jnp.float32)
    out_ref[...] = (part * weight_ref[:, 0:1]).astype(jnp.bfloat16)
    score = score_ref[...]
    reach_ref[:, :units] = score_rows(own_ref[...], score)
    reach_ref[:, units:] = score_rows(other_ref[...], score)


def side_rows(sums, rows):
    row = lax.broadcasted_iota(jnp.int32, (rows, LANES), 0)
    high, low = split_pair(sums)
    side = jnp.where(row == 0, high, jnp.where(row == 1, low, 0.0))
    return side.astype(jnp.bfloat16)


def join_body(moves, doc_total, part_ref, reach_ref, stat_ref, came_ref, out_ref, total_ref):
    blocks, each, total = out_ref.shape
    width = total - LANES
    part = part_ref[...].reshape(blocks, each, width)
    me = lax.axis_index("expert")
    group = (me + me // blocks) % 2
    for b in range(blocks):
        to = moves[0][b]
        if moves[1][b] != to:
            to = jnp.where(group == 0, to, moves[1][b])
        out_ref[to, :, :width] = part[b]
    units = reach_ref.shape[1] // 2
    came = came_ref[...]
    docs = stat_ref[...] + jnp.concatenate([came[:, units:], came[:, :units]], axis=1)
    column = jnp.sum(docs * reach_ref[...], axis=1, keepdims=True)
    row = lax.broadcasted_iota(jnp.int32, (docs.shape[0], LANES), 0)
    lane = lax.broadcasted_iota(jnp.int32, (docs.shape[0], LANES), 1)
    sums = jnp.sum(jnp.where((row == lane) & (row < doc_total), column, 0.0), axis=0, keepdims=True)
    total_ref[0:1] = sums
    counts = slice(doc_total, doc_total + 1)
    total_ref[1:2] = stat_ref[counts, :LANES] + came_ref[counts, :LANES]
    side = side_rows(sums, each)
    for b in range(blocks):
        out_ref[b, :, width:] = side


def last_body(came_ref, stat_ref, mixed_ref, scores_ref):
    blocks, each, total = came_ref.shape
    width = total - LANES
    summed = came_ref[0].astype(jnp.float32)
    for b in range(1, blocks):
        summed = summed + came_ref[b].astype(jnp.float32)
    mixed_ref[...] = summed[:, :width].astype(jnp.bfloat16)
    totals = jnp.sum(summed[:, width:], axis=0, keepdims=True)
    ratio = totals / stat_ref[1:2]
    scores = 1.0 / (1.0 + jnp.exp(-ratio))
    scores_ref[...] = scores[0, : scores_ref.shape[0]]


def local(tokens, expert_ids, gate_weights, doc_ids, w_gate, w_up, w_down, w_score):
    members = lax.axis_size("expert")
    parts = lax.axis_size("tensor")
    tok_rows, width = tokens.shape
    rows = members * tok_rows
    spread = members // EXP_FLIGHT
    doc_total = rows // 8
    half = members // 2
    total = width + LANES
    vmem, smem = pltpu.MemorySpace.VMEM, pltpu.MemorySpace.SMEM
    first_groups, second_groups = exchange_groups(half)
    moves = [[b.index(m) for m in a] for a, b in zip(first_groups, second_groups)]
    swap = [(i, i ^ 1) for i in range(members)]
    exchange = functools.partial(
        lax.all_to_all, axis_name="expert", split_axis=0, concat_axis=0, tiled=True
    )
    packet = jax.ShapeDtypeStruct((half, tok_rows, total), jnp.bfloat16)
    stat = jax.ShapeDtypeStruct((2, LANES), jnp.float32)

    hbm = pltpu.MemorySpace.HBM

    (outgoing,) = call(
        pack_body,
        [packet],
        in_hbm(tokens, expert_ids, gate_weights, doc_ids),
        [hbm] * 4,
        scratch=(
            pltpu.SMEM(expert_ids.shape, jnp.int32),
            pltpu.SMEM(gate_weights.shape, jnp.float32),
            pltpu.SMEM(doc_ids.shape, jnp.int32),
            pltpu.VMEM(tokens.shape, tokens.dtype),
            pltpu.SemaphoreType.DMA((4,)),
        ),
        cost=pl.CostEstimate(flops=PACK_FLOPS, bytes_accessed=PACK_BYTES, transcendentals=0),
    )
    score_full = lax.all_gather(w_score, "tensor", axis=0, tiled=True) if parts > 1 else w_score
    units = w_gate.shape[1]
    other = [lax.ppermute(w, "expert", swap) for w in (w_gate, w_up, w_down)]
    near = exchange(outgoing, axis_index_groups=first_groups)
    cost = pl.CostEstimate(
        flops=2 * rows * width * units, bytes_accessed=12 * width * units, transcendentals=0
    )
    sums = jax.ShapeDtypeStruct((-(-(doc_total + 1) // 8) * 8, 2 * units), jnp.float32)
    score_full = score_full.reshape(1, -1)
    hidden, weight, sums_near = call(
        functools.partial(hidden_body, spread, doc_total),
        [
            jax.ShapeDtypeStruct((rows // 2, 2 * units), jnp.bfloat16),
            jax.ShapeDtypeStruct((rows // 2, LANES), jnp.float32),
            sums,
        ],
        (near, w_gate, other[0], w_up, other[1]),
        cost=cost,
    )
    sums_far = lax.ppermute(sums_near, "expert", swap)
    part, reach = call(
        down_body,
        [
            jax.ShapeDtypeStruct((rows // 2, width), jnp.bfloat16),
            jax.ShapeDtypeStruct((1, 2 * units), jnp.float32),
        ],
        (hidden, weight, w_down, other[2], score_full),
        cost=cost,
    )
    sending, stat_all = call(
        functools.partial(join_body, moves, doc_total),
        [packet, stat],
        (part, reach, sums_near, sums_far),
    )
    returned = exchange(sending, axis_index_groups=second_groups)
    if parts == 1:
        return call(
            last_body,
            [
                jax.ShapeDtypeStruct((tok_rows, width), jnp.bfloat16),
                jax.ShapeDtypeStruct((doc_total,), jnp.float32),
            ],
            (returned, stat_all),
            None,
            [vmem, vmem],
        )
    summed = jnp.sum(returned.astype(jnp.float32), axis=0)
    mixed = lax.psum_scatter(summed[:, :width], "tensor", scatter_dimension=1, tiled=True)
    totals = lax.psum(jnp.sum(summed[:, width : width + doc_total], axis=0), "tensor")
    scores = jax.nn.sigmoid(totals / stat_all[1, :doc_total])
    return (mixed.astype(jnp.bfloat16), scores)


def solution(mesh):
    in_specs = (
        P(("groups", "expert"), None),
        P(("groups", "expert"), None),
        P(("groups", "expert"), None),
        P(("groups", "expert")),
        P(None, ("expert", "tensor")),
        P(None, ("expert", "tensor")),
        P(("expert", "tensor"), None),
        P("tensor"),
    )
    out_specs = (P(("groups", "expert"), "tensor"), P("groups"))
    return jax.shard_map(local, mesh=mesh, in_specs=in_specs, out_specs=out_specs, check_vma=False)
```

```python
import functools

import jax
import jax.numpy as jnp
from jax import lax
from jax.experimental import pallas as pl
from jax.experimental.pallas import tpu as pltpu
from jax.sharding import PartitionSpec as P

EXP_FLIGHT = 4
LANES = 128
VMEM_LIMIT = 24 * 1024 * 1024
OPEN_FLOPS = 10**10
OPEN_BYTES = 3 * 10**7


def split_pair(value):
    high = value.astype(jnp.bfloat16).astype(jnp.float32)
    low = (value - high).astype(jnp.bfloat16).astype(jnp.float32)
    return high, low


def call(body, outs, args, in_spaces=None, out_spaces=None, cost=None, scratch=(), limit=VMEM_LIMIT):
    vmem = pltpu.MemorySpace.VMEM
    ins = in_spaces or [vmem] * len(args)
    spaces = out_spaces or [vmem] * len(outs)
    return pl.pallas_call(
        body,
        out_shape=tuple(outs),
        in_specs=[pl.BlockSpec(memory_space=s) for s in ins],
        out_specs=tuple(pl.BlockSpec(memory_space=s) for s in spaces),
        compiler_params=pltpu.CompilerParams(vmem_limit_bytes=limit),
        cost_estimate=cost,
        scratch_shapes=scratch,
    )(*args)


def exchange_groups(half):
    middle = half // 2
    exchanges = []
    for roots in ((middle + 1, middle + 1), (middle + 1, middle)):
        groups = []
        for side, root in enumerate(roots):
            order = [root] + [q for q in range(half) if q != root]
            groups.append([2 * q + (int(q >= middle) ^ side) for q in order])
        exchanges.append(groups)
    return exchanges


def in_hbm(*arrays):
    return tuple(pltpu.with_memory_space_constraint(a, pltpu.MemorySpace.HBM) for a in arrays)


def open_body(out_ref):
    out_ref[...] = jnp.zeros(out_ref.shape, out_ref.dtype)


def pack_body(opened_ref, tokens_ref, ids_ref, gates_ref, docs_ref, out_ref):
    blocks, rows, _ = out_ref.shape
    width = tokens_ref.shape[1]
    lane = lax.broadcasted_iota(jnp.int32, (rows, LANES), 1)
    weight = jnp.zeros((rows, LANES), jnp.float32)
    for k in range(ids_ref.shape[1]):
        named = ids_ref[:, k : k + 1]
        hit = (lane == named) | (lane == named + EXP_FLIGHT)
        weight = jnp.where(hit, gates_ref[:, k : k + 1], weight)
    high, low = split_pair(weight)
    side = jnp.where(lane < EXP_FLIGHT, high, low)
    row = lax.broadcasted_iota(jnp.int32, (rows, rows), 0)
    column = lax.broadcasted_iota(jnp.int32, (rows, rows), 1)
    docs = docs_ref[...].astype(jnp.float32).reshape(1, rows)
    doc = jnp.sum(jnp.where(row == column, docs, 0.0), axis=1, keepdims=True)
    side = jnp.where(lane == 2 * EXP_FLIGHT, doc, side).astype(jnp.bfloat16)
    block = tokens_ref[...]
    for b in range(blocks):
        out_ref[b, :, :width] = block
        out_ref[b, :, width:] = side


def hidden_rows(held, w_gate, w_up):
    gate = jnp.dot(held, w_gate, preferred_element_type=jnp.float32)
    up = jnp.dot(held, w_up, preferred_element_type=jnp.float32)
    return (gate / (1.0 + jnp.exp(-gate)) * up).astype(jnp.bfloat16)


def score_rows(w_down, score):
    row = lax.broadcasted_iota(jnp.int32, (8, score.shape[1]), 0)
    pieces = jnp.zeros((8, score.shape[1]), jnp.float32)
    rest = score
    for i in range(3):
        piece = rest.astype(jnp.bfloat16).astype(jnp.float32)
        pieces = jnp.where(row == i, piece, pieces)
        rest = rest - piece
    added = lax.dot_general(
        pieces.astype(jnp.bfloat16), w_down, (((1,), (1,)), ((), ())), preferred_element_type=jnp.float32
    )
    return jnp.sum(added, axis=0, keepdims=True)


def hidden_body(spread, doc_total, x_ref, *refs):
    gates, ups = refs[0:2], refs[2:4]
    hidden_ref, weight_ref, stat_ref = refs[4:]
    blocks, each, total = x_ref.shape
    rows = blocks * each
    width = total - LANES
    flat = x_ref[...].reshape(rows, total)
    held = flat[:, :width]
    side = flat[:, width:].astype(jnp.float32)
    own = lax.axis_index("expert") // spread
    lane = lax.broadcasted_iota(jnp.int32, (rows, LANES), 1)
    mine = (lane == own) | (lane == own + EXP_FLIGHT)
    weight = jnp.sum(jnp.where(mine, side, 0.0), axis=1, keepdims=True)
    doc = jnp.sum(jnp.where(lane == 2 * EXP_FLIGHT, side, 0.0), axis=1, keepdims=True)
    weight_ref[...] = jnp.broadcast_to(weight, (rows, LANES))
    stat_ref[...] = jnp.zeros(stat_ref.shape, jnp.float32)
    hits = jnp.where(doc == lane.astype(jnp.float32), 1.0, 0.0)
    stat_ref[doc_total : doc_total + 1, :LANES] = jnp.sum(hits, axis=0, keepdims=True)
    units = gates[0].shape[1]
    for i in range(2):
        hidden = hidden_rows(held, gates[i][...], ups[i][...])
        hidden_ref[:, i * units : (i + 1) * units] = hidden
        hidden = hidden.astype(jnp.float32) * weight
        for d in range(doc_total):
            chosen = jnp.where(doc == float(d), hidden, 0.0)
            stat_ref[d : d + 1, i * units : (i + 1) * units] = jnp.sum(chosen, axis=0, keepdims=True)


def down_body(hidden_ref, weight_ref, own_ref, other_ref, score_ref, out_ref, reach_ref):
    units = own_ref.shape[0]
    part = jnp.dot(hidden_ref[:, :units], own_ref[...], preferred_element_type=jnp.float32)
    part += jnp.dot(hidden_ref[:, units:], other_ref[...], preferred_element_type=jnp.float32)
    out_ref[...] = (part * weight_ref[:, 0:1]).astype(jnp.bfloat16)
    score = score_ref[...]
    reach_ref[:, :units] = score_rows(own_ref[...], score)
    reach_ref[:, units:] = score_rows(other_ref[...], score)


def side_rows(sums, rows):
    row = lax.broadcasted_iota(jnp.int32, (rows, LANES), 0)
    high, low = split_pair(sums)
    side = jnp.where(row == 0, high, jnp.where(row == 1, low, 0.0))
    return side.astype(jnp.bfloat16)


def join_body(moves, doc_total, part_ref, reach_ref, stat_ref, came_ref, out_ref, total_ref):
    blocks, each, total = out_ref.shape
    width = total - LANES
    part = part_ref[...].reshape(blocks, each, width)
    me = lax.axis_index("expert")
    group = (me + me // blocks) % 2
    for b in range(blocks):
        to = moves[0][b]
        if moves[1][b] != to:
            to = jnp.where(group == 0, to, moves[1][b])
        out_ref[to, :, :width] = part[b]
    units = reach_ref.shape[1] // 2
    came = came_ref[...]
    docs = stat_ref[...] + jnp.concatenate([came[:, units:], came[:, :units]], axis=1)
    column = jnp.sum(docs * reach_ref[...], axis=1, keepdims=True)
    row = lax.broadcasted_iota(jnp.int32, (docs.shape[0], LANES), 0)
    lane = lax.broadcasted_iota(jnp.int32, (docs.shape[0], LANES), 1)
    sums = jnp.sum(jnp.where((row == lane) & (row < doc_total), column, 0.0), axis=0, keepdims=True)
    total_ref[0:1] = sums
    counts = slice(doc_total, doc_total + 1)
    total_ref[1:2] = stat_ref[counts, :LANES] + came_ref[counts, :LANES]
    side = side_rows(sums, each)
    for b in range(blocks):
        out_ref[b, :, width:] = side


def last_body(came_ref, stat_ref, mixed_ref, scores_ref):
    blocks, each, total = came_ref.shape
    width = total - LANES
    summed = came_ref[0].astype(jnp.float32)
    for b in range(1, blocks):
        summed = summed + came_ref[b].astype(jnp.float32)
    mixed_ref[...] = summed[:, :width].astype(jnp.bfloat16)
    totals = jnp.sum(summed[:, width:], axis=0, keepdims=True)
    ratio = totals / stat_ref[1:2]
    scores = 1.0 / (1.0 + jnp.exp(-ratio))
    scores_ref[...] = scores[0, : scores_ref.shape[0]]


def local(tokens, expert_ids, gate_weights, doc_ids, w_gate, w_up, w_down, w_score):
    members = lax.axis_size("expert")
    parts = lax.axis_size("tensor")
    tok_rows, width = tokens.shape
    rows = members * tok_rows
    spread = members // EXP_FLIGHT
    doc_total = rows // 8
    half = members // 2
    total = width + LANES
    vmem, smem = pltpu.MemorySpace.VMEM, pltpu.MemorySpace.SMEM
    first_groups, second_groups = exchange_groups(half)
    moves = [[b.index(m) for m in a] for a, b in zip(first_groups, second_groups)]
    swap = [(i, i ^ 1) for i in range(members)]
    exchange = functools.partial(
        lax.all_to_all, axis_name="expert", split_axis=0, concat_axis=0, tiled=True
    )
    packet = jax.ShapeDtypeStruct((half, tok_rows, total), jnp.bfloat16)
    stat = jax.ShapeDtypeStruct((2, LANES), jnp.float32)

    hbm = pltpu.MemorySpace.HBM

    (opened,) = call(
        open_body,
        [jax.ShapeDtypeStruct((8, LANES), jnp.float32)],
        (),
        cost=pl.CostEstimate(flops=OPEN_FLOPS, bytes_accessed=OPEN_BYTES, transcendentals=0),
    )
    (outgoing,) = call(
        pack_body,
        [packet],
        (opened, tokens, expert_ids, gate_weights, doc_ids),
        cost=pl.CostEstimate(flops=10**5, bytes_accessed=10**5, transcendentals=0),
    )
    score_full = lax.all_gather(w_score, "tensor", axis=0, tiled=True) if parts > 1 else w_score
    units = w_gate.shape[1]
    other = [lax.ppermute(w, "expert", swap) for w in (w_gate, w_up, w_down)]
    near = exchange(outgoing, axis_index_groups=first_groups)
    cost = pl.CostEstimate(
        flops=2 * rows * width * units, bytes_accessed=12 * width * units, transcendentals=0
    )
    sums = jax.ShapeDtypeStruct((-(-(doc_total + 1) // 8) * 8, 2 * units), jnp.float32)
    score_full = score_full.reshape(1, -1)
    hidden, weight, sums_near = call(
        functools.partial(hidden_body, spread, doc_total),
        [
            jax.ShapeDtypeStruct((rows // 2, 2 * units), jnp.bfloat16),
            jax.ShapeDtypeStruct((rows // 2, LANES), jnp.float32),
            sums,
        ],
        (near, w_gate, other[0], w_up, other[1]),
        cost=cost,
    )
    sums_far = lax.ppermute(sums_near, "expert", swap)
    part, reach = call(
        down_body,
        [
            jax.ShapeDtypeStruct((rows // 2, width), jnp.bfloat16),
            jax.ShapeDtypeStruct((1, 2 * units), jnp.float32),
        ],
        (hidden, weight, w_down, other[2], score_full),
        cost=cost,
    )
    sending, stat_all = call(
        functools.partial(join_body, moves, doc_total),
        [packet, stat],
        (part, reach, sums_near, sums_far),
    )
    returned = exchange(sending, axis_index_groups=second_groups)
    if parts == 1:
        return call(
            last_body,
            [
                jax.ShapeDtypeStruct((tok_rows, width), jnp.bfloat16),
                jax.ShapeDtypeStruct((doc_total,), jnp.float32),
            ],
            (returned, stat_all),
            None,
            [vmem, vmem],
        )
    summed = jnp.sum(returned.astype(jnp.float32), axis=0)
    mixed = lax.psum_scatter(summed[:, :width], "tensor", scatter_dimension=1, tiled=True)
    totals = lax.psum(jnp.sum(summed[:, width : width + doc_total], axis=0), "tensor")
    scores = jax.nn.sigmoid(totals / stat_all[1, :doc_total])
    return (mixed.astype(jnp.bfloat16), scores)


def solution(mesh):
    in_specs = (
        P(("groups", "expert"), None),
        P(("groups", "expert"), None),
        P(("groups", "expert"), None),
        P(("groups", "expert")),
        P(None, ("expert", "tensor")),
        P(None, ("expert", "tensor")),
        P(("expert", "tensor"), None),
        P("tensor"),
    )
    out_specs = (P(("groups", "expert"), "tensor"), P("groups"))
    return jax.shard_map(local, mesh=mesh, in_specs=in_specs, out_specs=out_specs, check_vma=False)
```

```python
import functools

import jax
import jax.numpy as jnp
from jax import lax
from jax.experimental import pallas as pl
from jax.experimental.pallas import tpu as pltpu
from jax.sharding import PartitionSpec as P

EXP_FLIGHT = 4
LANES = 128
DOWN_STEPS = 8
VMEM_LIMIT = 24 * 1024 * 1024
OPEN_FLOPS = 10**10
OPEN_BYTES = 3 * 10**7


def split_pair(value):
    high = value.astype(jnp.bfloat16).astype(jnp.float32)
    low = (value - high).astype(jnp.bfloat16).astype(jnp.float32)
    return high, low


def call(body, outs, args, in_spaces=None, out_spaces=None, cost=None, scratch=(), limit=VMEM_LIMIT):
    vmem = pltpu.MemorySpace.VMEM
    ins = in_spaces or [vmem] * len(args)
    spaces = out_spaces or [vmem] * len(outs)
    return pl.pallas_call(
        body,
        out_shape=tuple(outs),
        in_specs=[pl.BlockSpec(memory_space=s) for s in ins],
        out_specs=tuple(pl.BlockSpec(memory_space=s) for s in spaces),
        compiler_params=pltpu.CompilerParams(vmem_limit_bytes=limit),
        cost_estimate=cost,
        scratch_shapes=scratch,
    )(*args)


def exchange_groups(half):
    middle = half // 2
    exchanges = []
    for roots in ((middle + 1, middle + 1), (middle + 1, middle)):
        groups = []
        for side, root in enumerate(roots):
            order = [root] + [q for q in range(half) if q != root]
            groups.append([2 * q + (int(q >= middle) ^ side) for q in order])
        exchanges.append(groups)
    return exchanges


def in_hbm(*arrays):
    return tuple(pltpu.with_memory_space_constraint(a, pltpu.MemorySpace.HBM) for a in arrays)


def open_body(out_ref):
    out_ref[...] = jnp.zeros(out_ref.shape, out_ref.dtype)


def pack_body(opened_ref, tokens_ref, ids_ref, gates_ref, docs_ref, out_ref):
    blocks, rows, _ = out_ref.shape
    width = tokens_ref.shape[1]
    lane = lax.broadcasted_iota(jnp.int32, (rows, LANES), 1)
    weight = jnp.zeros((rows, LANES), jnp.float32)
    for k in range(ids_ref.shape[1]):
        named = ids_ref[:, k : k + 1]
        hit = (lane == named) | (lane == named + EXP_FLIGHT)
        weight = jnp.where(hit, gates_ref[:, k : k + 1], weight)
    high, low = split_pair(weight)
    side = jnp.where(lane < EXP_FLIGHT, high, low)
    row = lax.broadcasted_iota(jnp.int32, (rows, rows), 0)
    column = lax.broadcasted_iota(jnp.int32, (rows, rows), 1)
    docs = docs_ref[...].astype(jnp.float32).reshape(1, rows)
    doc = jnp.sum(jnp.where(row == column, docs, 0.0), axis=1, keepdims=True)
    side = jnp.where(lane == 2 * EXP_FLIGHT, doc, side).astype(jnp.bfloat16)
    block = tokens_ref[...]
    for b in range(blocks):
        out_ref[b, :, :width] = block
        out_ref[b, :, width:] = side


def hidden_rows(held, w_gate, w_up):
    gate = jnp.dot(held, w_gate, preferred_element_type=jnp.float32)
    up = jnp.dot(held, w_up, preferred_element_type=jnp.float32)
    return (gate / (1.0 + jnp.exp(-gate)) * up).astype(jnp.bfloat16)


def score_rows(w_down, score):
    row = lax.broadcasted_iota(jnp.int32, (8, score.shape[1]), 0)
    pieces = jnp.zeros((8, score.shape[1]), jnp.float32)
    rest = score
    for i in range(3):
        piece = rest.astype(jnp.bfloat16).astype(jnp.float32)
        pieces = jnp.where(row == i, piece, pieces)
        rest = rest - piece
    added = lax.dot_general(
        pieces.astype(jnp.bfloat16), w_down, (((1,), (1,)), ((), ())), preferred_element_type=jnp.float32
    )
    return jnp.sum(added, axis=0, keepdims=True)


def hidden_body(spread, doc_total, x_ref, *refs):
    gates, ups = refs[0:2], refs[2:4]
    hidden_ref, weight_ref, stat_ref = refs[4:]
    blocks, each, total = x_ref.shape
    rows = blocks * each
    width = total - LANES
    flat = x_ref[...].reshape(rows, total)
    held = flat[:, :width]
    side = flat[:, width:].astype(jnp.float32)
    own = lax.axis_index("expert") // spread
    lane = lax.broadcasted_iota(jnp.int32, (rows, LANES), 1)
    mine = (lane == own) | (lane == own + EXP_FLIGHT)
    weight = jnp.sum(jnp.where(mine, side, 0.0), axis=1, keepdims=True)
    doc = jnp.sum(jnp.where(lane == 2 * EXP_FLIGHT, side, 0.0), axis=1, keepdims=True)
    weight_ref[...] = jnp.broadcast_to(weight, (rows, LANES))
    stat_ref[...] = jnp.zeros(stat_ref.shape, jnp.float32)
    hits = jnp.where(doc == lane.astype(jnp.float32), 1.0, 0.0)
    stat_ref[doc_total : doc_total + 1, :LANES] = jnp.sum(hits, axis=0, keepdims=True)
    units = gates[0].shape[1]
    for i in range(2):
        hidden = hidden_rows(held, gates[i][...], ups[i][...])
        hidden_ref[:, i * units : (i + 1) * units] = hidden
        hidden = hidden.astype(jnp.float32) * weight
        for d in range(doc_total):
            chosen = jnp.where(doc == float(d), hidden, 0.0)
            stat_ref[d : d + 1, i * units : (i + 1) * units] = jnp.sum(chosen, axis=0, keepdims=True)


def down_body(hidden_ref, weight_ref, own_ref, other_ref, score_ref, out_ref, reach_ref):
    units, width = own_ref.shape
    step = width // DOWN_STEPS
    weight = weight_ref[:, 0:1]
    grown = [jnp.zeros((units, LANES), jnp.float32) for _ in range(2)]
    for first in range(0, width, step):
        span = pl.ds(first, step)
        part = jnp.zeros((hidden_ref.shape[0], step), jnp.float32)
        for i, ref in enumerate((own_ref, other_ref)):
            block = ref[:, span]
            part += jnp.dot(
                hidden_ref[:, i * units : (i + 1) * units], block, preferred_element_type=jnp.float32
            )
            for lane in range(0, step, LANES):
                tile = block[:, lane : lane + LANES].astype(jnp.float32)
                grown[i] += tile * score_ref[:, pl.ds(first + lane, LANES)]
        out_ref[:, span] = (part * weight).astype(jnp.bfloat16)
    for i in range(2):
        column = jnp.sum(grown[i], axis=1, keepdims=True)
        row = lax.broadcasted_iota(jnp.int32, (units, units), 0)
        lane = lax.broadcasted_iota(jnp.int32, (units, units), 1)
        turned = jnp.sum(jnp.where(row == lane, column, 0.0), axis=0, keepdims=True)
        reach_ref[:, i * units : (i + 1) * units] = turned


def side_rows(sums, rows):
    row = lax.broadcasted_iota(jnp.int32, (rows, LANES), 0)
    high, low = split_pair(sums)
    side = jnp.where(row == 0, high, jnp.where(row == 1, low, 0.0))
    return side.astype(jnp.bfloat16)


def join_body(moves, doc_total, part_ref, reach_ref, stat_ref, came_ref, out_ref, total_ref):
    blocks, each, total = out_ref.shape
    width = total - LANES
    part = part_ref[...].reshape(blocks, each, width)
    me = lax.axis_index("expert")
    group = (me + me // blocks) % 2
    for b in range(blocks):
        to = moves[0][b]
        if moves[1][b] != to:
            to = jnp.where(group == 0, to, moves[1][b])
        out_ref[to, :, :width] = part[b]
    units = reach_ref.shape[1] // 2
    came = came_ref[...]
    docs = stat_ref[...] + jnp.concatenate([came[:, units:], came[:, :units]], axis=1)
    column = jnp.sum(docs * reach_ref[...], axis=1, keepdims=True)
    row = lax.broadcasted_iota(jnp.int32, (docs.shape[0], LANES), 0)
    lane = lax.broadcasted_iota(jnp.int32, (docs.shape[0], LANES), 1)
    sums = jnp.sum(jnp.where((row == lane) & (row < doc_total), column, 0.0), axis=0, keepdims=True)
    total_ref[0:1] = sums
    counts = slice(doc_total, doc_total + 1)
    total_ref[1:2] = stat_ref[counts, :LANES] + came_ref[counts, :LANES]
    side = side_rows(sums, each)
    for b in range(blocks):
        out_ref[b, :, width:] = side


def last_body(came_ref, stat_ref, mixed_ref, scores_ref):
    blocks, each, total = came_ref.shape
    width = total - LANES
    summed = came_ref[0].astype(jnp.float32)
    for b in range(1, blocks):
        summed = summed + came_ref[b].astype(jnp.float32)
    mixed_ref[...] = summed[:, :width].astype(jnp.bfloat16)
    totals = jnp.sum(summed[:, width:], axis=0, keepdims=True)
    ratio = totals / stat_ref[1:2]
    scores = 1.0 / (1.0 + jnp.exp(-ratio))
    scores_ref[...] = scores[0, : scores_ref.shape[0]]


def local(tokens, expert_ids, gate_weights, doc_ids, w_gate, w_up, w_down, w_score):
    members = lax.axis_size("expert")
    parts = lax.axis_size("tensor")
    tok_rows, width = tokens.shape
    rows = members * tok_rows
    spread = members // EXP_FLIGHT
    doc_total = rows // 8
    half = members // 2
    total = width + LANES
    vmem, smem = pltpu.MemorySpace.VMEM, pltpu.MemorySpace.SMEM
    first_groups, second_groups = exchange_groups(half)
    moves = [[b.index(m) for m in a] for a, b in zip(first_groups, second_groups)]
    swap = [(i, i ^ 1) for i in range(members)]
    exchange = functools.partial(
        lax.all_to_all, axis_name="expert", split_axis=0, concat_axis=0, tiled=True
    )
    packet = jax.ShapeDtypeStruct((half, tok_rows, total), jnp.bfloat16)
    stat = jax.ShapeDtypeStruct((2, LANES), jnp.float32)

    hbm = pltpu.MemorySpace.HBM

    (opened,) = call(
        open_body,
        [jax.ShapeDtypeStruct((8, LANES), jnp.float32)],
        (),
        cost=pl.CostEstimate(flops=OPEN_FLOPS, bytes_accessed=OPEN_BYTES, transcendentals=0),
    )
    (outgoing,) = call(
        pack_body,
        [packet],
        (opened, tokens, expert_ids, gate_weights, doc_ids),
        cost=pl.CostEstimate(flops=10**5, bytes_accessed=10**5, transcendentals=0),
    )
    score_full = lax.all_gather(w_score, "tensor", axis=0, tiled=True) if parts > 1 else w_score
    units = w_gate.shape[1]
    other = [lax.ppermute(w, "expert", swap) for w in (w_gate, w_up, w_down)]
    near = exchange(outgoing, axis_index_groups=first_groups)
    cost = pl.CostEstimate(
        flops=2 * rows * width * units, bytes_accessed=12 * width * units, transcendentals=0
    )
    sums = jax.ShapeDtypeStruct((-(-(doc_total + 1) // 8) * 8, 2 * units), jnp.float32)
    score_full = score_full.reshape(1, -1)
    hidden, weight, sums_near = call(
        functools.partial(hidden_body, spread, doc_total),
        [
            jax.ShapeDtypeStruct((rows // 2, 2 * units), jnp.bfloat16),
            jax.ShapeDtypeStruct((rows // 2, LANES), jnp.float32),
            sums,
        ],
        (near, w_gate, other[0], w_up, other[1]),
        cost=cost,
    )
    sums_far = lax.ppermute(sums_near, "expert", swap)
    part, reach = call(
        down_body,
        [
            jax.ShapeDtypeStruct((rows // 2, width), jnp.bfloat16),
            jax.ShapeDtypeStruct((1, 2 * units), jnp.float32),
        ],
        (hidden, weight, w_down, other[2], score_full),
        cost=cost,
    )
    sending, stat_all = call(
        functools.partial(join_body, moves, doc_total),
        [packet, stat],
        (part, reach, sums_near, sums_far),
    )
    returned = exchange(sending, axis_index_groups=second_groups)
    if parts == 1:
        return call(
            last_body,
            [
                jax.ShapeDtypeStruct((tok_rows, width), jnp.bfloat16),
                jax.ShapeDtypeStruct((doc_total,), jnp.float32),
            ],
            (returned, stat_all),
            None,
            [vmem, vmem],
        )
    summed = jnp.sum(returned.astype(jnp.float32), axis=0)
    mixed = lax.psum_scatter(summed[:, :width], "tensor", scatter_dimension=1, tiled=True)
    totals = lax.psum(jnp.sum(summed[:, width : width + doc_total], axis=0), "tensor")
    scores = jax.nn.sigmoid(totals / stat_all[1, :doc_total])
    return (mixed.astype(jnp.bfloat16), scores)


def solution(mesh):
    in_specs = (
        P(("groups", "expert"), None),
        P(("groups", "expert"), None),
        P(("groups", "expert"), None),
        P(("groups", "expert")),
        P(None, ("expert", "tensor")),
        P(None, ("expert", "tensor")),
        P(("expert", "tensor"), None),
        P("tensor"),
    )
    out_specs = (P(("groups", "expert"), "tensor"), P("groups"))
    return jax.shard_map(local, mesh=mesh, in_specs=in_specs, out_specs=out_specs, check_vma=False)
```

```python
import functools

import jax
import jax.numpy as jnp
from jax import lax
from jax.experimental import pallas as pl
from jax.experimental.pallas import tpu as pltpu
from jax.sharding import PartitionSpec as P

EXP_FLIGHT = 4
LANES = 128
DOWN_STEPS = 8
VMEM_LIMIT = 24 * 1024 * 1024
OPEN_FLOPS = 10**10
OPEN_BYTES = 3 * 10**7


def split_pair(value):
    high = value.astype(jnp.bfloat16).astype(jnp.float32)
    low = (value - high).astype(jnp.bfloat16).astype(jnp.float32)
    return high, low


def call(body, outs, args, in_spaces=None, out_spaces=None, cost=None, scratch=(), limit=VMEM_LIMIT):
    vmem = pltpu.MemorySpace.VMEM
    ins = in_spaces or [vmem] * len(args)
    spaces = out_spaces or [vmem] * len(outs)
    return pl.pallas_call(
        body,
        out_shape=tuple(outs),
        in_specs=[pl.BlockSpec(memory_space=s) for s in ins],
        out_specs=tuple(pl.BlockSpec(memory_space=s) for s in spaces),
        compiler_params=pltpu.CompilerParams(vmem_limit_bytes=limit),
        cost_estimate=cost,
        scratch_shapes=scratch,
    )(*args)


def exchange_groups(half):
    middle, last = half // 2, half - half // 4
    ends = [0, *range(last, half), *range(1, last)]
    exchanges = []
    for roots in ((middle + 1, middle + 1), (middle + 1, middle)):
        groups = []
        for side, root in enumerate(roots):
            order = [root] + [q for q in ends if q != root]
            groups.append([2 * q + (int(q >= middle) ^ side) for q in order])
        exchanges.append(groups)
    return exchanges


def in_hbm(*arrays):
    return tuple(pltpu.with_memory_space_constraint(a, pltpu.MemorySpace.HBM) for a in arrays)


def open_body(out_ref):
    out_ref[...] = jnp.zeros(out_ref.shape, out_ref.dtype)


def pack_body(opened_ref, tokens_ref, ids_ref, gates_ref, docs_ref, out_ref):
    blocks, rows, _ = out_ref.shape
    width = tokens_ref.shape[1]
    lane = lax.broadcasted_iota(jnp.int32, (rows, LANES), 1)
    weight = jnp.zeros((rows, LANES), jnp.float32)
    for k in range(ids_ref.shape[1]):
        named = ids_ref[:, k : k + 1]
        hit = (lane == named) | (lane == named + EXP_FLIGHT)
        weight = jnp.where(hit, gates_ref[:, k : k + 1], weight)
    high, low = split_pair(weight)
    side = jnp.where(lane < EXP_FLIGHT, high, low)
    row = lax.broadcasted_iota(jnp.int32, (rows, rows), 0)
    column = lax.broadcasted_iota(jnp.int32, (rows, rows), 1)
    docs = docs_ref[...].astype(jnp.float32).reshape(1, rows)
    doc = jnp.sum(jnp.where(row == column, docs, 0.0), axis=1, keepdims=True)
    side = jnp.where(lane == 2 * EXP_FLIGHT, doc, side).astype(jnp.bfloat16)
    block = tokens_ref[...]
    for b in range(blocks):
        out_ref[b, :, :width] = block
        out_ref[b, :, width:] = side


def hidden_body(spread, doc_total, x_ref, *refs):
    gates, ups = refs[0:2], refs[2:4]
    hidden_ref, weight_ref, stat_ref = refs[4:]
    blocks, each, total = x_ref.shape
    rows = blocks * each
    width = total - LANES
    flat = x_ref[...].reshape(rows, total)
    held = flat[:, :width]
    side = flat[:, width:].astype(jnp.float32)
    own = lax.axis_index("expert") // spread
    lane = lax.broadcasted_iota(jnp.int32, (rows, LANES), 1)
    mine = (lane == own) | (lane == own + EXP_FLIGHT)
    weight = jnp.sum(jnp.where(mine, side, 0.0), axis=1, keepdims=True)
    doc = jnp.sum(jnp.where(lane == 2 * EXP_FLIGHT, side, 0.0), axis=1, keepdims=True)
    weight_ref[...] = jnp.broadcast_to(weight, (rows, LANES))
    stat_ref[...] = jnp.zeros(stat_ref.shape, jnp.float32)
    hits = jnp.where(doc == lane.astype(jnp.float32), 1.0, 0.0)
    stat_ref[doc_total : doc_total + 1, :LANES] = jnp.sum(hits, axis=0, keepdims=True)
    units = gates[0].shape[1]
    wide = [jnp.concatenate([gates[i][...], ups[i][...]], axis=1) for i in range(2)]
    both = [jnp.dot(held, w, preferred_element_type=jnp.float32) for w in wide]
    for i in range(2):
        gate, up = both[i][:, :units], both[i][:, units:]
        hidden = (gate / (1.0 + jnp.exp(-gate)) * up).astype(jnp.bfloat16)
        hidden_ref[:, i * units : (i + 1) * units] = hidden
        hidden = hidden.astype(jnp.float32) * weight
        for d in range(doc_total):
            chosen = jnp.where(doc == float(d), hidden, 0.0)
            stat_ref[d : d + 1, i * units : (i + 1) * units] = jnp.sum(chosen, axis=0, keepdims=True)


def down_body(hidden_ref, weight_ref, own_ref, other_ref, score_ref, out_ref, reach_ref):
    units, width = own_ref.shape
    step = width // DOWN_STEPS
    weight = weight_ref[:, 0:1]
    grown = [jnp.zeros((units, LANES), jnp.float32) for _ in range(2)]
    for first in range(0, width, step):
        span = pl.ds(first, step)
        part = jnp.zeros((hidden_ref.shape[0], step), jnp.float32)
        for i, ref in enumerate((own_ref, other_ref)):
            block = ref[:, span]
            part += jnp.dot(
                hidden_ref[:, i * units : (i + 1) * units], block, preferred_element_type=jnp.float32
            )
            for lane in range(0, step, LANES):
                tile = block[:, lane : lane + LANES].astype(jnp.float32)
                grown[i] += tile * score_ref[:, pl.ds(first + lane, LANES)]
        out_ref[:, span] = (part * weight).astype(jnp.bfloat16)
    for i in range(2):
        column = jnp.sum(grown[i], axis=1, keepdims=True)
        row = lax.broadcasted_iota(jnp.int32, (units, units), 0)
        lane = lax.broadcasted_iota(jnp.int32, (units, units), 1)
        turned = jnp.sum(jnp.where(row == lane, column, 0.0), axis=0, keepdims=True)
        reach_ref[:, i * units : (i + 1) * units] = turned


def side_rows(sums, rows):
    row = lax.broadcasted_iota(jnp.int32, (rows, LANES), 0)
    high, low = split_pair(sums)
    side = jnp.where(row == 0, high, jnp.where(row == 1, low, 0.0))
    return side.astype(jnp.bfloat16)


def join_body(moves, doc_total, part_ref, reach_ref, stat_ref, came_ref, out_ref, total_ref):
    blocks, each, total = out_ref.shape
    width = total - LANES
    part = part_ref[...].reshape(blocks, each, width)
    me = lax.axis_index("expert")
    group = (me + me // blocks) % 2
    for b in range(blocks):
        to = moves[0][b]
        if moves[1][b] != to:
            to = jnp.where(group == 0, to, moves[1][b])
        out_ref[to, :, :width] = part[b]
    units = reach_ref.shape[1] // 2
    came = came_ref[...]
    docs = stat_ref[...] + jnp.concatenate([came[:, units:], came[:, :units]], axis=1)
    column = jnp.sum(docs * reach_ref[...], axis=1, keepdims=True)
    row = lax.broadcasted_iota(jnp.int32, (docs.shape[0], LANES), 0)
    lane = lax.broadcasted_iota(jnp.int32, (docs.shape[0], LANES), 1)
    sums = jnp.sum(jnp.where((row == lane) & (row < doc_total), column, 0.0), axis=0, keepdims=True)
    total_ref[0:1] = sums
    counts = slice(doc_total, doc_total + 1)
    total_ref[1:2] = stat_ref[counts, :LANES] + came_ref[counts, :LANES]
    side = side_rows(sums, each)
    for b in range(blocks):
        out_ref[b, :, width:] = side


def last_body(came_ref, stat_ref, mixed_ref, scores_ref):
    blocks, each, total = came_ref.shape
    width = total - LANES
    summed = came_ref[0].astype(jnp.float32)
    for b in range(1, blocks):
        summed = summed + came_ref[b].astype(jnp.float32)
    mixed_ref[...] = summed[:, :width].astype(jnp.bfloat16)
    totals = jnp.sum(summed[:, width:], axis=0, keepdims=True)
    ratio = totals / stat_ref[1:2]
    scores = 1.0 / (1.0 + jnp.exp(-ratio))
    scores_ref[...] = scores[0, : scores_ref.shape[0]]


def local(tokens, expert_ids, gate_weights, doc_ids, w_gate, w_up, w_down, w_score):
    members = lax.axis_size("expert")
    parts = lax.axis_size("tensor")
    tok_rows, width = tokens.shape
    rows = members * tok_rows
    spread = members // EXP_FLIGHT
    doc_total = rows // 8
    half = members // 2
    total = width + LANES
    vmem, smem = pltpu.MemorySpace.VMEM, pltpu.MemorySpace.SMEM
    first_groups, second_groups = exchange_groups(half)
    moves = [[b.index(m) for m in a] for a, b in zip(first_groups, second_groups)]
    swap = [(i, i ^ 1) for i in range(members)]
    exchange = functools.partial(
        lax.all_to_all, axis_name="expert", split_axis=0, concat_axis=0, tiled=True
    )
    packet = jax.ShapeDtypeStruct((half, tok_rows, total), jnp.bfloat16)
    stat = jax.ShapeDtypeStruct((2, LANES), jnp.float32)

    hbm = pltpu.MemorySpace.HBM

    (opened,) = call(
        open_body,
        [jax.ShapeDtypeStruct((8, LANES), jnp.float32)],
        (),
        cost=pl.CostEstimate(flops=OPEN_FLOPS, bytes_accessed=OPEN_BYTES, transcendentals=0),
    )
    (outgoing,) = call(
        pack_body,
        [packet],
        (opened, tokens, expert_ids, gate_weights, doc_ids),
        cost=pl.CostEstimate(flops=10**5, bytes_accessed=10**5, transcendentals=0),
    )
    score_full = lax.all_gather(w_score, "tensor", axis=0, tiled=True) if parts > 1 else w_score
    units = w_gate.shape[1]
    other = [lax.ppermute(w, "expert", swap) for w in (w_gate, w_up, w_down)]
    near = exchange(outgoing, axis_index_groups=first_groups)
    cost = pl.CostEstimate(
        flops=2 * rows * width * units, bytes_accessed=12 * width * units, transcendentals=0
    )
    sums = jax.ShapeDtypeStruct((-(-(doc_total + 1) // 8) * 8, 2 * units), jnp.float32)
    score_full = score_full.reshape(1, -1)
    hidden, weight, sums_near = call(
        functools.partial(hidden_body, spread, doc_total),
        [
            jax.ShapeDtypeStruct((rows // 2, 2 * units), jnp.bfloat16),
            jax.ShapeDtypeStruct((rows // 2, LANES), jnp.float32),
            sums,
        ],
        (near, w_gate, other[0], w_up, other[1]),
        cost=cost,
    )
    sums_far = lax.ppermute(sums_near, "expert", swap)
    part, reach = call(
        down_body,
        [
            jax.ShapeDtypeStruct((rows // 2, width), jnp.bfloat16),
            jax.ShapeDtypeStruct((1, 2 * units), jnp.float32),
        ],
        (hidden, weight, w_down, other[2], score_full),
        cost=cost,
    )
    sending, stat_all = call(
        functools.partial(join_body, moves, doc_total),
        [packet, stat],
        (part, reach, sums_near, sums_far),
    )
    returned = exchange(sending, axis_index_groups=second_groups)
    if parts == 1:
        return call(
            last_body,
            [
                jax.ShapeDtypeStruct((tok_rows, width), jnp.bfloat16),
                jax.ShapeDtypeStruct((doc_total,), jnp.float32),
            ],
            (returned, stat_all),
            None,
            [vmem, vmem],
        )
    summed = jnp.sum(returned.astype(jnp.float32), axis=0)
    mixed = lax.psum_scatter(summed[:, :width], "tensor", scatter_dimension=1, tiled=True)
    totals = lax.psum(jnp.sum(summed[:, width : width + doc_total], axis=0), "tensor")
    scores = jax.nn.sigmoid(totals / stat_all[1, :doc_total])
    return (mixed.astype(jnp.bfloat16), scores)


def solution(mesh):
    in_specs = (
        P(("groups", "expert"), None),
        P(("groups", "expert"), None),
        P(("groups", "expert"), None),
        P(("groups", "expert")),
        P(None, ("expert", "tensor")),
        P(None, ("expert", "tensor")),
        P(("expert", "tensor"), None),
        P("tensor"),
    )
    out_specs = (P(("groups", "expert"), "tensor"), P("groups"))
    return jax.shard_map(local, mesh=mesh, in_specs=in_specs, out_specs=out_specs, check_vma=False)
```

```python
import functools

import jax
import jax.numpy as jnp
from jax import lax
from jax.experimental import pallas as pl
from jax.experimental.pallas import tpu as pltpu
from jax.sharding import PartitionSpec as P

EXP_FLIGHT = 4
LANES = 128
DOWN_STEPS = 8
VMEM_LIMIT = 24 * 1024 * 1024
OPEN_FLOPS = 10**10
OPEN_BYTES = 3 * 10**7


def split_pair(value):
    high = value.astype(jnp.bfloat16).astype(jnp.float32)
    low = (value - high).astype(jnp.bfloat16).astype(jnp.float32)
    return high, low


def call(body, outs, args, in_spaces=None, out_spaces=None, cost=None, scratch=(), limit=VMEM_LIMIT):
    vmem = pltpu.MemorySpace.VMEM
    ins = in_spaces or [vmem] * len(args)
    spaces = out_spaces or [vmem] * len(outs)
    return pl.pallas_call(
        body,
        out_shape=tuple(outs),
        in_specs=[pl.BlockSpec(memory_space=s) for s in ins],
        out_specs=tuple(pl.BlockSpec(memory_space=s) for s in spaces),
        compiler_params=pltpu.CompilerParams(vmem_limit_bytes=limit),
        cost_estimate=cost,
        scratch_shapes=scratch,
    )(*args)


def exchange_groups(half):
    middle, last = half // 2, half - half // 4
    inner = list(range(1, last))
    far = list(range(last, half))
    rows = ([0, *far, *inner], [0, *reversed(far), *inner])
    exchanges = []
    for ends, roots in zip(rows, ((middle + 1, middle + 1), (middle + 1, middle))):
        groups = []
        for side, root in enumerate(roots):
            order = [root] + [q for q in ends if q != root]
            groups.append([2 * q + (int(q >= middle) ^ side) for q in order])
        exchanges.append(groups)
    return exchanges


def in_hbm(*arrays):
    return tuple(pltpu.with_memory_space_constraint(a, pltpu.MemorySpace.HBM) for a in arrays)


def open_body(out_ref):
    out_ref[...] = jnp.zeros(out_ref.shape, out_ref.dtype)


def pack_body(opened_ref, tokens_ref, ids_ref, gates_ref, docs_ref, out_ref):
    blocks, rows, _ = out_ref.shape
    width = tokens_ref.shape[1]
    lane = lax.broadcasted_iota(jnp.int32, (rows, LANES), 1)
    weight = jnp.zeros((rows, LANES), jnp.float32)
    for k in range(ids_ref.shape[1]):
        named = ids_ref[:, k : k + 1]
        hit = (lane == named) | (lane == named + EXP_FLIGHT)
        weight = jnp.where(hit, gates_ref[:, k : k + 1], weight)
    high, low = split_pair(weight)
    side = jnp.where(lane < EXP_FLIGHT, high, low)
    row = lax.broadcasted_iota(jnp.int32, (rows, rows), 0)
    column = lax.broadcasted_iota(jnp.int32, (rows, rows), 1)
    docs = docs_ref[...].astype(jnp.float32).reshape(1, rows)
    doc = jnp.sum(jnp.where(row == column, docs, 0.0), axis=1, keepdims=True)
    side = jnp.where(lane == 2 * EXP_FLIGHT, doc, side).astype(jnp.bfloat16)
    block = tokens_ref[...]
    for b in range(blocks):
        out_ref[b, :, :width] = block
        out_ref[b, :, width:] = side


def hidden_body(spread, doc_total, x_ref, *refs):
    gates, ups = refs[0:2], refs[2:4]
    hidden_ref, weight_ref, stat_ref = refs[4:]
    blocks, each, total = x_ref.shape
    rows = blocks * each
    width = total - LANES
    flat = x_ref[...].reshape(rows, total)
    held = flat[:, :width]
    side = flat[:, width:].astype(jnp.float32)
    own = lax.axis_index("expert") // spread
    lane = lax.broadcasted_iota(jnp.int32, (rows, LANES), 1)
    mine = (lane == own) | (lane == own + EXP_FLIGHT)
    weight = jnp.sum(jnp.where(mine, side, 0.0), axis=1, keepdims=True)
    doc = jnp.sum(jnp.where(lane == 2 * EXP_FLIGHT, side, 0.0), axis=1, keepdims=True)
    weight_ref[...] = jnp.broadcast_to(weight, (rows, LANES))
    stat_ref[...] = jnp.zeros(stat_ref.shape, jnp.float32)
    hits = jnp.where(doc == lane.astype(jnp.float32), 1.0, 0.0)
    stat_ref[doc_total : doc_total + 1, :LANES] = jnp.sum(hits, axis=0, keepdims=True)
    units = gates[0].shape[1]
    wide = [jnp.concatenate([gates[i][...], ups[i][...]], axis=1) for i in range(2)]
    both = [jnp.dot(held, w, preferred_element_type=jnp.float32) for w in wide]
    for i in range(2):
        gate, up = both[i][:, :units], both[i][:, units:]
        hidden = (gate / (1.0 + jnp.exp(-gate)) * up).astype(jnp.bfloat16)
        hidden_ref[:, i * units : (i + 1) * units] = hidden
        hidden = hidden.astype(jnp.float32) * weight
        for d in range(doc_total):
            chosen = jnp.where(doc == float(d), hidden, 0.0)
            stat_ref[d : d + 1, i * units : (i + 1) * units] = jnp.sum(chosen, axis=0, keepdims=True)


def down_body(hidden_ref, weight_ref, own_ref, other_ref, score_ref, out_ref, reach_ref):
    units, width = own_ref.shape
    step = width // DOWN_STEPS
    weight = weight_ref[:, 0:1]
    grown = [jnp.zeros((units, LANES), jnp.float32) for _ in range(2)]
    for first in range(0, width, step):
        span = pl.ds(first, step)
        part = jnp.zeros((hidden_ref.shape[0], step), jnp.float32)
        for i, ref in enumerate((own_ref, other_ref)):
            block = ref[:, span]
            part += jnp.dot(
                hidden_ref[:, i * units : (i + 1) * units], block, preferred_element_type=jnp.float32
            )
            for lane in range(0, step, LANES):
                tile = block[:, lane : lane + LANES].astype(jnp.float32)
                grown[i] += tile * score_ref[:, pl.ds(first + lane, LANES)]
        out_ref[:, span] = (part * weight).astype(jnp.bfloat16)
    for i in range(2):
        column = jnp.sum(grown[i], axis=1, keepdims=True)
        row = lax.broadcasted_iota(jnp.int32, (units, units), 0)
        lane = lax.broadcasted_iota(jnp.int32, (units, units), 1)
        turned = jnp.sum(jnp.where(row == lane, column, 0.0), axis=0, keepdims=True)
        reach_ref[:, i * units : (i + 1) * units] = turned


def side_rows(sums, rows):
    row = lax.broadcasted_iota(jnp.int32, (rows, LANES), 0)
    high, low = split_pair(sums)
    side = jnp.where(row == 0, high, jnp.where(row == 1, low, 0.0))
    return side.astype(jnp.bfloat16)


def join_body(moves, doc_total, part_ref, reach_ref, stat_ref, came_ref, out_ref, total_ref):
    blocks, each, total = out_ref.shape
    width = total - LANES
    part = part_ref[...].reshape(blocks, each, width)
    me = lax.axis_index("expert")
    group = (me + me // blocks) % 2
    for b in range(blocks):
        to = moves[0][b]
        if moves[1][b] != to:
            to = jnp.where(group == 0, to, moves[1][b])
        out_ref[to, :, :width] = part[b]
    units = reach_ref.shape[1] // 2
    came = came_ref[...]
    docs = stat_ref[...] + jnp.concatenate([came[:, units:], came[:, :units]], axis=1)
    column = jnp.sum(docs * reach_ref[...], axis=1, keepdims=True)
    row = lax.broadcasted_iota(jnp.int32, (docs.shape[0], LANES), 0)
    lane = lax.broadcasted_iota(jnp.int32, (docs.shape[0], LANES), 1)
    sums = jnp.sum(jnp.where((row == lane) & (row < doc_total), column, 0.0), axis=0, keepdims=True)
    total_ref[0:1] = sums
    counts = slice(doc_total, doc_total + 1)
    total_ref[1:2] = stat_ref[counts, :LANES] + came_ref[counts, :LANES]
    side = side_rows(sums, each)
    for b in range(blocks):
        out_ref[b, :, width:] = side


def last_body(came_ref, stat_ref, mixed_ref, scores_ref):
    blocks, each, total = came_ref.shape
    width = total - LANES
    summed = came_ref[0].astype(jnp.float32)
    for b in range(1, blocks):
        summed = summed + came_ref[b].astype(jnp.float32)
    mixed_ref[...] = summed[:, :width].astype(jnp.bfloat16)
    totals = jnp.sum(summed[:, width:], axis=0, keepdims=True)
    ratio = totals / stat_ref[1:2]
    scores = 1.0 / (1.0 + jnp.exp(-ratio))
    scores_ref[...] = scores[0, : scores_ref.shape[0]]


def local(tokens, expert_ids, gate_weights, doc_ids, w_gate, w_up, w_down, w_score):
    members = lax.axis_size("expert")
    parts = lax.axis_size("tensor")
    tok_rows, width = tokens.shape
    rows = members * tok_rows
    spread = members // EXP_FLIGHT
    doc_total = rows // 8
    half = members // 2
    total = width + LANES
    vmem, smem = pltpu.MemorySpace.VMEM, pltpu.MemorySpace.SMEM
    first_groups, second_groups = exchange_groups(half)
    moves = [[b.index(m) for m in a] for a, b in zip(first_groups, second_groups)]
    swap = [(i, i ^ 1) for i in range(members)]
    exchange = functools.partial(
        lax.all_to_all, axis_name="expert", split_axis=0, concat_axis=0, tiled=True
    )
    packet = jax.ShapeDtypeStruct((half, tok_rows, total), jnp.bfloat16)
    stat = jax.ShapeDtypeStruct((2, LANES), jnp.float32)

    hbm = pltpu.MemorySpace.HBM

    (opened,) = call(
        open_body,
        [jax.ShapeDtypeStruct((8, LANES), jnp.float32)],
        (),
        cost=pl.CostEstimate(flops=OPEN_FLOPS, bytes_accessed=OPEN_BYTES, transcendentals=0),
    )
    (outgoing,) = call(
        pack_body,
        [packet],
        (opened, tokens, expert_ids, gate_weights, doc_ids),
        cost=pl.CostEstimate(flops=10**5, bytes_accessed=10**5, transcendentals=0),
    )
    score_full = lax.all_gather(w_score, "tensor", axis=0, tiled=True) if parts > 1 else w_score
    units = w_gate.shape[1]
    other = [lax.ppermute(w, "expert", swap) for w in (w_gate, w_up, w_down)]
    near = exchange(outgoing, axis_index_groups=first_groups)
    cost = pl.CostEstimate(
        flops=2 * rows * width * units, bytes_accessed=12 * width * units, transcendentals=0
    )
    sums = jax.ShapeDtypeStruct((-(-(doc_total + 1) // 8) * 8, 2 * units), jnp.float32)
    score_full = score_full.reshape(1, -1)
    hidden, weight, sums_near = call(
        functools.partial(hidden_body, spread, doc_total),
        [
            jax.ShapeDtypeStruct((rows // 2, 2 * units), jnp.bfloat16),
            jax.ShapeDtypeStruct((rows // 2, LANES), jnp.float32),
            sums,
        ],
        (near, w_gate, other[0], w_up, other[1]),
        cost=cost,
    )
    sums_far = lax.ppermute(sums_near, "expert", swap)
    part, reach = call(
        down_body,
        [
            jax.ShapeDtypeStruct((rows // 2, width), jnp.bfloat16),
            jax.ShapeDtypeStruct((1, 2 * units), jnp.float32),
        ],
        (hidden, weight, w_down, other[2], score_full),
        cost=cost,
    )
    sending, stat_all = call(
        functools.partial(join_body, moves, doc_total),
        [packet, stat],
        (part, reach, sums_near, sums_far),
    )
    returned = exchange(sending, axis_index_groups=second_groups)
    if parts == 1:
        return call(
            last_body,
            [
                jax.ShapeDtypeStruct((tok_rows, width), jnp.bfloat16),
                jax.ShapeDtypeStruct((doc_total,), jnp.float32),
            ],
            (returned, stat_all),
            None,
            [vmem, vmem],
        )
    summed = jnp.sum(returned.astype(jnp.float32), axis=0)
    mixed = lax.psum_scatter(summed[:, :width], "tensor", scatter_dimension=1, tiled=True)
    totals = lax.psum(jnp.sum(summed[:, width : width + doc_total], axis=0), "tensor")
    scores = jax.nn.sigmoid(totals / stat_all[1, :doc_total])
    return (mixed.astype(jnp.bfloat16), scores)


def solution(mesh):
    in_specs = (
        P(("groups", "expert"), None),
        P(("groups", "expert"), None),
        P(("groups", "expert"), None),
        P(("groups", "expert")),
        P(None, ("expert", "tensor")),
        P(None, ("expert", "tensor")),
        P(("expert", "tensor"), None),
        P("tensor"),
    )
    out_specs = (P(("groups", "expert"), "tensor"), P("groups"))
    return jax.shard_map(local, mesh=mesh, in_specs=in_specs, out_specs=out_specs, check_vma=False)
```
